32 devices in a mesh: grp: 2 (over y), seq: 8 (over z, x), tp: 2 (over core).
Axes of the slice: x: 2, y: 2, z: 4, core: 2. Of those that a mesh axis runs over, the one named last changes fastest.
Arguments:
- queries: bfloat16 [4096, 2048], P(('grp', 'seq'), 'tp'), parts along dimension 0, may hold values from -9 to 9
- keys: bfloat16 [4096, 2048], P(('grp', 'seq'), 'tp'), parts along dimension 0, may hold values from -9 to 9
- values: bfloat16 [4096, 2048], P(('grp', 'seq'), 'tp'), parts along dimension 0, may hold values from -18 to 18
- segment_ids: int32 [4096], P(('grp', 'seq')), parts along dimension 0, may hold values from 0 to 7, never falling along the last dimension, each value on 1 to 512 neighbouring positions
- modality: int32 [4096], P(('grp', 'seq')), parts along dimension 0, may hold values 0 or 1
- norm_gain: float32 [2, 2048], P(None, 'tp'), may hold values from 0.1 to 1.9
Outputs:
- blended: bfloat16 [4096, 2048], P(('grp', 'seq'), 'tp'), parts along dimension 0
The draws below stay inside these ranges and needn't reach their ends.
There are 2 independent parts, one for each index of `grp`. The reference program is written for one: setup_inputs(seed, part) draws one part's arguments, and reference() takes and returns one part's arrays. A program takes and returns all parts, laid end to end along the dimension named above; an argument that names none is the same for every part. Nothing has to cross between parts.
Inputs may be any that keep to these rules, and one draw needn't show every extreme that they name: `segment_ids`: ids never fall along the sequence; each document holds 1 to 512 tokens, and one holds exactly that many.
All inputs are finite; a program needn't handle non-finite values. No bound on the sum of `modality` on one device may be relied on, other than what follows from the above.
Results may differ from the reference program's by a relative error of at most 0.009.
Values may be sent and summed in bfloat16 or wider, within the bound.
A program may use at most 64 MiB of HBM per device.

```python
import math
import jax
import jax.numpy as jnp
import numpy as np
from jax import lax

HEADS = 16
HEAD_DIM = 128
TOK_DEV = 256
REACH = 2
TOKENS = 2048
DOCS = 8
N_SEQ = 8


def draw_entries(key, part):
    key_base = jax.random.fold_in(key, 7)
    key_query, key_other = jax.random.split(key_base, 2)
    array_shape = (TOKENS, HEADS * HEAD_DIM)
    query_draw = jnp.clip(jax.random.normal(key_query, array_shape, jnp.float32), -6.0, 6.0)
    key_draw = jnp.clip(jax.random.normal(key_other, array_shape, jnp.float32), -6.0, 6.0)
    return (query_draw, key_draw)


def draw_queries(key, part):
    return draw_entries(key, part)[0].astype(jnp.bfloat16)


def draw_keys(key, part):
    return draw_entries(key, part)[1].astype(jnp.bfloat16)


def draw_values(key, part):
    key_base = jax.random.fold_in(key, 11)
    key_entry, key_scale = jax.random.split(key_base, 2)
    array_shape = (TOKENS, HEADS * HEAD_DIM)
    entries = jnp.clip(jax.random.normal(key_entry, array_shape, jnp.float32), -6.0, 6.0)
    head_scale = jnp.exp(jax.random.uniform(key_scale, (HEADS,), jnp.float32, jnp.log(0.3), jnp.log(3.0)))
    column_scale = jnp.repeat(head_scale, HEAD_DIM)
    return (entries * column_scale[None, :]).astype(jnp.bfloat16)


def touch_ends(values, key, low, largest):
    place = [jax.random.randint(jax.random.fold_in(key, axis), (), 0, length) for axis, length in enumerate(values.shape)]
    main_axis = values.shape.index(max(values.shape))
    beside = place[:main_axis] + [(place[main_axis] + 1) % values.shape[main_axis]] + place[main_axis + 1:]
    return values.at[tuple(place)].set(low).at[tuple(beside)].set(largest)


def profile(number_of, total, limit, slope):
    weights = [(1 << 20) // math.isqrt(grade ** slope) + 1 for grade in range(2, number_of + 1)]
    spare, holding = total - limit - (number_of - 1), [1] * (number_of - 1)
    while spare > 0:
        candidates = [i for i in range(number_of - 1) if holding[i] < limit]
        pool, left = sum([weights[i] for i in candidates]), spare
        for i in candidates:
            extra = min(limit - holding[i], max(1, left * weights[i] // pool), spare)
            holding[i] = holding[i] + extra
            spare = spare - extra
    return np.array([limit] + holding)


def uneven(stream_key, count, total, bound, slope):
    if count == 2:
        one = jax.random.randint(stream_key, (), max(1, total - bound), min(bound, total - 1) + 1)
        return jnp.stack([one, total - one])
    tallies = jnp.asarray(profile(count, total, bound, slope), jnp.int32)
    pairs = (count - 1) // 2
    source_of, receiver = tallies[1:1 + 2 * pairs:2], tallies[2:2 + 2 * pairs:2]
    room = jnp.minimum(source_of - 1, bound - receiver)
    shifted = jax.random.randint(jax.random.fold_in(stream_key, 1), (pairs,), 0, 1 << 20) % (room + 1)
    tallies = tallies.at[1:1 + 2 * pairs:2].set(source_of - shifted).at[2:2 + 2 * pairs:2].set(receiver + shifted)
    return tallies[jax.random.permutation(jax.random.fold_in(stream_key, 2), count)]


def setup_inputs(seed: int = 0, part: int = 0) -> dict:
    streams_of = jax.random.split(jax.random.key(seed), 7)
    own_keys = jax.random.split(jax.random.fold_in(streams_of[6], part), 7)
    return {
        "queries": draw_queries(jax.random.fold_in(jax.random.fold_in(streams_of[6], part), 71), part),
        "keys": draw_keys(jax.random.fold_in(jax.random.fold_in(streams_of[6], part), 71), part),
        "values": draw_values(jax.random.fold_in(jax.random.fold_in(streams_of[6], part), 71), part),
        "segment_ids": jnp.searchsorted(jnp.cumsum(uneven(own_keys[3], DOCS, TOKENS, REACH * TOK_DEV, 1)), jnp.arange(TOKENS), side="right").astype(jnp.int32),
        "modality": touch_ends((jax.random.randint(own_keys[4], (TOKENS,), 0, 2) < 1).astype(jnp.int32), jax.random.fold_in(own_keys[4], 1), 0, 1),
        "norm_gain": jnp.clip(1.0 + 0.18 * jax.random.normal(streams_of[5], (2, HEADS * HEAD_DIM), jnp.float32), 0.1, 1.9),
    }


def attend_block(block_index, queries, keys, values, segment_ids):
    key_span = (REACH + 1) * TOK_DEV
    first_key = (jnp.maximum(block_index - REACH, 0) * TOK_DEV).astype(jnp.int32)
    first_query = (block_index * TOK_DEV).astype(jnp.int32)
    q_rows = lax.dynamic_slice_in_dim(queries, first_query, TOK_DEV, 0).astype(jnp.float32).reshape(TOK_DEV, HEADS, HEAD_DIM)
    k_rows = lax.dynamic_slice_in_dim(keys, first_key, key_span, 0).astype(jnp.float32).reshape(key_span, HEADS, HEAD_DIM)
    v_rows = lax.dynamic_slice_in_dim(values, first_key, key_span, 0).astype(jnp.float32).reshape(key_span, HEADS, HEAD_DIM)
    query_segs = lax.dynamic_slice_in_dim(segment_ids, first_query, TOK_DEV, 0)
    key_segs = lax.dynamic_slice_in_dim(segment_ids, first_key, key_span, 0)
    query_pos = first_query + jnp.arange(TOK_DEV, dtype=jnp.int32)
    key_pos = first_key + jnp.arange(key_span, dtype=jnp.int32)
    allowed = (query_segs[:, None] == key_segs[None, :]) & (key_pos[None, :] <= query_pos[:, None])
    scores = jnp.einsum('qhd,khd->hqk', q_rows, k_rows) * HEAD_DIM ** (-0.5)
    scores = jnp.where(allowed[None], scores, -jnp.inf)
    row_max = lax.optimization_barrier(jnp.max(scores, axis=2, keepdims=True))
    weights = jnp.exp(scores - row_max)
    row_total = lax.optimization_barrier(jnp.sum(weights, axis=2))
    rounded = weights.astype(jnp.bfloat16).astype(jnp.float32)
    summed = jnp.einsum('hqk,khd->qhd', rounded, v_rows)
    attended = summed / jnp.transpose(row_total)[:, :, None]
    return attended.reshape(TOK_DEV, HEADS * HEAD_DIM).astype(jnp.bfloat16)

def reference(queries, keys, values, segment_ids, modality, norm_gain):
    indices = jnp.arange(N_SEQ, dtype=jnp.int32)
    attended = lax.map(lambda block_index: attend_block(block_index, queries, keys, values, segment_ids), indices)
    attended = attended.reshape(TOKENS, HEADS * HEAD_DIM).astype(jnp.float32)
    mean_square = lax.optimization_barrier(jnp.sum(attended * attended, axis=1)) / (HEADS * HEAD_DIM)
    gain_rows = jnp.where((modality == 1)[:, None], norm_gain[1][None, :], norm_gain[0][None, :])
    blended = attended * lax.rsqrt(mean_square + 1e-05)[:, None] * gain_rows
    return blended.astype(jnp.bfloat16)
```

```python
import functools

import jax
import jax.numpy as jnp
from jax import lax
from jax.experimental import pallas as pl
from jax.experimental.pallas import tpu as pltpu
from jax.sharding import PartitionSpec as P

HEADS = 16
HEAD_DIM = 128
REACH = 2
MESH = pl.DeviceIdType.MESH
PIECES = 4
DIRECT = (2, 2)
RELAY = 1


def kernel(
    n,
    heads,
    rows,
    q_hbm,
    k_hbm,
    v_hbm,
    seg_hbm,
    mod_hbm,
    att,
    inverse_ref,
    image_ref,
    q_own,
    own,
    buf1,
    buf2,
    hop,
    seg_ref,
    mod_ref,
    seg1,
    seg2,
    bias,
    squares,
    mine,
    theirs,
    in_sem,
    send_a,
    send_b,
    send_c,
    recv_1,
    recv_2,
    hop_send,
    hop_recv,
    id_sem,
    seg_send,
    seg_recv,
    sq_sem,
):
    s = lax.axis_index("seq")
    t = lax.axis_index("tp")
    even = lax.rem(s, 2) == 0
    odd = lax.rem(s, 2) == 1
    has_next = s + 2 < n
    has_prev = s >= 2
    ahead = odd & (s + 1 < n)
    passes = even & has_next & (t == RELAY)
    behind = even & has_prev
    pair = s + 1 - 2 * lax.rem(s, 2)

    half = PIECES // 2
    depth = rows // half

    def columns_of(h):
        return pl.ds(h * HEAD_DIM, HEAD_DIM)

    def load_piece(h, p):
        source = k_hbm if p < half else v_hbm
        piece = pl.ds((p % half) * depth, depth)
        return pltpu.make_async_copy(
            source.at[piece, columns_of(h)], own.at[h, p], in_sem.at[h, p]
        )

    def load_q(h):
        return pltpu.make_async_copy(q_hbm.at[:, columns_of(h)], q_own.at[h], in_sem.at[h, PIECES])

    last = heads - 1
    count = jnp.where(t == 0, DIRECT[0], DIRECT[1])
    most = max(DIRECT)
    tail = range(PIECES - most, PIECES)
    relay = t == RELAY

    def is_direct(p):
        return p >= PIECES - count

    def load_ids(i):
        source, target = ((seg_hbm, seg_ref), (mod_hbm, mod_ref))[i]
        return pltpu.make_async_copy(source, target, id_sem.at[i])

    barrier = pltpu.get_barrier_semaphore()
    across = (odd & ~relay & (s + 1 < n)) | (even & relay & has_next)
    onward = even & relay & has_next
    inward = even & ~relay & has_prev
    peers = (
        (None, {"tp": 1 - t}),
        (None, {"seq": pair}),
        (has_next, {"seq": s + 2}),
        (has_prev, {"seq": s - 2}),
        (across, {"seq": pair, "tp": 1 - t}),
        (onward, {"seq": s + 2, "tp": 1 - t}),
        (inward, {"seq": s - 2, "tp": 1 - t}),
    )
    expected = 0
    for condition, peer in peers:

        def greet(peer=peer):
            pl.semaphore_signal(barrier, inc=1, device_id=peer, device_id_type=MESH)

        if condition is None:
            greet()
            expected = expected + 1
        else:
            pl.when(condition)(greet)
            expected = expected + jnp.where(condition, 1, 0)

    for p in tail:
        load_piece(last, p).start()
    load_ids(0).start()
    for h in range(heads):
        for p in range(PIECES):
            if h < last or p not in tail:
                load_piece(h, p).start()
    load_ids(1).start()
    load_ids(0).wait()
    pl.semaphore_wait(barrier, expected)

    def remote(source, target, send, recv, where, core=t):
        return pltpu.make_async_remote_copy(
            src_ref=source,
            dst_ref=target,
            send_sem=send,
            recv_sem=recv,
            device_id={"seq": where, "tp": core},
            device_id_type=MESH,
        )

    def flow_a(h, p):
        return remote(own.at[h, p], buf1.at[h, p], send_a, recv_1.at[h, p], pair)

    def flow_b(h, p):
        return remote(own.at[h, p], buf2.at[h, p], send_b, recv_2.at[h, p], s + 2)

    def flow_c(h, p):
        return remote(buf2.at[h, p], buf1.at[h, p], send_c.at[h], recv_1.at[h, p], pair)

    def flow_d(p):
        i = p - tail[0]
        return remote(
            own.at[last, p], hop.at[t, i], hop_send.at[t, i], hop_recv.at[t, i], pair, RELAY
        )

    def flow_e(p, core):
        i = p - tail[0]
        return remote(
            hop.at[core, i],
            buf1.at[last, p],
            hop_send.at[core, i],
            recv_1.at[last, p],
            s + 2,
            core,
        )

    def hop_in(p, core):
        i = p - tail[0]
        return remote(
            own.at[last, p], hop.at[core, i], hop_send.at[core, i], hop_recv.at[core, i], pair
        )

    def direct_of(core):
        return range(PIECES - DIRECT[core], PIECES)

    def forwards(h, p):
        if p not in tail:
            return odd & has_prev
        return odd & has_prev & ((h < last) | ~is_direct(p))

    def seg_a():
        return remote(seg_ref, seg1, seg_send.at[0], seg_recv.at[0], pair)

    def seg_b():
        return remote(seg_ref, seg2, seg_send.at[1], seg_recv.at[1], s + 2)

    def seg_c():
        return remote(seg2, seg1, seg_send.at[2], seg_recv.at[0], pair)

    @pl.when(even)
    def _():
        seg_a().start()

    @pl.when(has_next)
    def _():
        seg_b().start()

    for p in tail:
        load_piece(last, p).wait()

        @pl.when(ahead & is_direct(p))
        def _():
            flow_d(p).start()

    def send_pieces(h, waits):
        for p in range(PIECES):
            if p in waits:
                load_piece(h, p).wait()

            @pl.when(has_next)
            def _():
                flow_b(h, p).start()

            @pl.when(even)
            def _():
                flow_a(h, p).start()

        load_q(h).start()

    def send(h, carry):
        send_pieces(h, range(PIECES))
        return carry

    lax.fori_loop(0, last, send, 0)
    send_pieces(last, range(PIECES - most))
    load_ids(1).wait()

    @pl.when(s < 1)
    def _():
        buf1[...] = jnp.zeros_like(buf1)
        seg1[...] = jnp.full_like(seg1, -1)

    @pl.when(s < 2)
    def _():
        buf2[...] = jnp.zeros_like(buf2)
        seg2[...] = jnp.full_like(seg2, -1)

    def column(row):
        return jnp.transpose(jnp.broadcast_to(row, (HEAD_DIM, rows)))

    query_seg = column(seg_ref[...])[:, :1]
    query_pos = lax.broadcasted_iota(jnp.int32, (rows, rows), 0)
    key_pos = lax.broadcasted_iota(jnp.int32, (rows, rows), 1)
    allowed = (query_seg == seg_ref[...]) & (key_pos <= query_pos)
    bias[:, :rows] = jnp.where(allowed, 0.0, -jnp.inf)
    squares[...] = jnp.zeros_like(squares)
    image_ref[...] = column(mod_ref[...])

    @pl.when(has_prev)
    def _():
        seg_b().wait_recv()

    @pl.when(odd & has_prev)
    def _():
        seg_c().start()

    @pl.when(s >= 1)
    def _():
        seg_a().wait_recv()

    bias[:, rows : 2 * rows] = jnp.where(query_seg == seg1[...], 0.0, -jnp.inf)
    bias[:, 2 * rows :] = jnp.where(query_seg == seg2[...], 0.0, -jnp.inf)

    @pl.when(passes)
    def _():
        for core in (0, 1):
            for p in direct_of(core):
                hop_in(p, core).wait_recv()
                flow_e(p, core).start()

    def scores_of(query, key):
        return lax.dot_general(
            query, key, (((1,), (1,)), ((), ())), preferred_element_type=jnp.float32
        )

    def arrive(h, pieces):
        for p in pieces:

            @pl.when(s >= 1)
            def _():
                flow_a(h, p).wait_recv()

    def head(h, pieces_apart):
        load_q(h).wait()
        query = q_own[h]
        scale = HEAD_DIM ** (-0.5)

        def scores_with(block, i):
            key = block[h, :half].reshape(rows, HEAD_DIM)
            return scores_of(query, key) * scale + bias[:, i * rows : (i + 1) * rows]

        def product(weight, block):
            value = block[h, half:].reshape(rows, HEAD_DIM)
            return jnp.dot(
                weight.astype(jnp.bfloat16), value, preferred_element_type=jnp.float32
            )

        for p in range(half):

            @pl.when(has_prev)
            def _():
                flow_b(h, p).wait_recv()

            @pl.when(forwards(h, p))
            def _():
                flow_c(h, p).start()

        @pl.when(odd & has_prev)
        def _():
            for p in range(half, PIECES):
                flow_b(h, p).wait_recv()

                @pl.when(forwards(h, p))
                def _():
                    flow_c(h, p).start()

        near = scores_with(own, 0)
        far = scores_with(buf2, 2)
        arrive(h, range(half))
        middle = scores_with(buf1, 1)
        top = jnp.max(jnp.maximum(jnp.maximum(near, middle), far), axis=1, keepdims=True)
        near = jnp.exp(near - top)
        far = jnp.exp(far - top)
        middle = jnp.exp(middle - top)
        total = jnp.sum(near + middle + far, axis=1, keepdims=True)
        acc = product(near, own)

        @pl.when(behind)
        def _():
            for p in range(half, PIECES):
                flow_b(h, p).wait_recv()

        if pieces_apart:
            acc = acc + product(far, buf2)
            inverse = 1.0 / total
            middle = middle.astype(jnp.bfloat16)
            for p in range(half, PIECES):
                arrive(h, (p,))
                part = middle[:, (p - half) * depth : (p - half + 1) * depth]
                acc = acc + jnp.dot(part, buf1[h, p], preferred_element_type=jnp.float32)
            attended = (acc * inverse).astype(jnp.bfloat16)
        else:
            arrive(h, range(half, PIECES))
            acc = acc + product(far, buf2) + product(middle, buf1)
            attended = (acc * (1.0 / total)).astype(jnp.bfloat16)
        att[h] = attended
        wide = attended.astype(jnp.float32)
        return wide * wide

    def one(h, carry):
        squares[...] += head(h, False)
        return carry

    lax.fori_loop(0, last, one, 0)
    partial = jnp.sum(squares[...] + head(last, True), axis=1, keepdims=True)
    mine[...] = jnp.broadcast_to(partial, mine.shape)
    swap = pltpu.make_async_remote_copy(
        src_ref=mine,
        dst_ref=theirs,
        send_sem=sq_sem.at[0],
        recv_sem=sq_sem.at[1],
        device_id={"tp": 1 - t},
        device_id_type=MESH,
    )
    swap.start()

    for p in tail:

        @pl.when(ahead & is_direct(p))
        def _():
            flow_d(p).wait_send()

    @pl.when(passes)
    def _():
        for core in (0, 1):
            for p in direct_of(core):
                flow_e(p, core).wait_send()

    @pl.when(even)
    def _():
        seg_a().wait_send()
        remote(own, own, send_a, recv_1.at[0, 0], pair).wait_send()

    @pl.when(has_next)
    def _():
        seg_b().wait_send()
        remote(own, own, send_b, recv_1.at[0, 0], pair).wait_send()

    @pl.when(odd & has_prev)
    def _():
        seg_c().wait_send()
        for h in range(last):
            remote(buf2.at[h], buf1.at[h], send_c.at[h], recv_1.at[h, 0], pair).wait_send()

    for p in range(PIECES):

        @pl.when(forwards(last, p))
        def _():
            flow_c(last, p).wait_send()

    swap.wait_recv()
    mean_square = (mine[...] + theirs[...]) / (HEADS * HEAD_DIM)
    inverse_ref[...] = lax.rsqrt(mean_square + 1e-05)
    swap.wait_send()


def blend(heads, att, inverse_ref, image_ref, gain_ref, out_hbm, staged, out_sem):
    inverse = inverse_ref[...]
    image = image_ref[...] == 1
    copies = []
    for h in range(heads):
        columns = slice(h * HEAD_DIM, (h + 1) * HEAD_DIM)
        gain = jnp.where(image, gain_ref[1:2, columns], gain_ref[0:1, columns])
        staged[h] = (att[h].astype(jnp.float32) * inverse * gain).astype(staged.dtype)
        copy = pltpu.make_async_copy(
            staged.at[h], out_hbm.at[:, pl.ds(h * HEAD_DIM, HEAD_DIM)], out_sem.at[h]
        )
        copy.start()
        copies.append(copy)
    for copy in copies:
        copy.wait()


def on_device(n, queries, keys, values, segment_ids, modality, norm_gain):
    rows, width = queries.shape
    heads = width // HEAD_DIM
    vmem = pl.BlockSpec(memory_space=pltpu.VMEM)
    hbm = pl.BlockSpec(memory_space=pltpu.HBM)
    depth = 2 * rows // PIECES
    block = pltpu.VMEM((heads, PIECES, depth, HEAD_DIM), jnp.bfloat16)
    flow = pltpu.SemaphoreType.DMA((heads, PIECES))
    att, inverse, image = pl.pallas_call(
        functools.partial(kernel, n, heads, rows),
        out_shape=(
            pltpu.VMEM((heads, rows, HEAD_DIM), jnp.bfloat16),
            pltpu.VMEM((rows, HEAD_DIM), jnp.float32),
            pltpu.VMEM((rows, HEAD_DIM), jnp.int32),
        ),
        in_specs=[hbm, hbm, hbm, hbm, hbm],
        out_specs=(vmem, vmem, vmem),
        scratch_shapes=[
            pltpu.VMEM((heads, rows, HEAD_DIM), jnp.bfloat16),
            block,
            block,
            block,
            pltpu.VMEM((2, max(DIRECT), depth, HEAD_DIM), jnp.bfloat16),
            pltpu.VMEM((1, rows), jnp.int32),
            pltpu.VMEM((1, rows), jnp.int32),
            pltpu.VMEM((1, rows), jnp.int32),
            pltpu.VMEM((1, rows), jnp.int32),
            pltpu.VMEM((rows, (REACH + 1) * rows), jnp.float32),
            pltpu.VMEM((rows, HEAD_DIM), jnp.float32),
            pltpu.VMEM((rows, HEAD_DIM), jnp.float32),
            pltpu.VMEM((rows, HEAD_DIM), jnp.float32),
            pltpu.SemaphoreType.DMA((heads, PIECES + 1)),
            pltpu.SemaphoreType.DMA,
            pltpu.SemaphoreType.DMA,
            pltpu.SemaphoreType.DMA((heads,)),
            flow,
            flow,
            pltpu.SemaphoreType.DMA((2, max(DIRECT))),
            pltpu.SemaphoreType.DMA((2, max(DIRECT))),
            pltpu.SemaphoreType.DMA((2,)),
            pltpu.SemaphoreType.DMA((3,)),
            pltpu.SemaphoreType.DMA((2,)),
            pltpu.SemaphoreType.DMA((2,)),
        ],
        compiler_params=pltpu.CompilerParams(
            collective_id=0, has_side_effects=True
        ),
    )(queries, keys, values, segment_ids.reshape(1, rows), modality.reshape(1, rows))
    return pl.pallas_call(
        functools.partial(blend, heads),
        out_shape=jax.ShapeDtypeStruct((rows, width), jnp.bfloat16),
        in_specs=[vmem, vmem, vmem, vmem],
        out_specs=hbm,
        scratch_shapes=[
            pltpu.VMEM((heads, rows, HEAD_DIM), jnp.bfloat16),
            pltpu.SemaphoreType.DMA((heads,)),
        ],
        compiler_params=pltpu.CompilerParams(vmem_limit_bytes=8 * 2**20),
    )(att, inverse, image, norm_gain)


def solution(mesh):
    return jax.shard_map(
        functools.partial(on_device, mesh.shape["seq"]),
        mesh=mesh,
        in_specs=(
            P(("grp", "seq"), "tp"),
            P(("grp", "seq"), "tp"),
            P(("grp", "seq"), "tp"),
            P(("grp", "seq")),
            P(("grp", "seq")),
            P(None, "tp"),
        ),
        out_specs=P(("grp", "seq"), "tp"),
        check_vma=False,
    )
```

```python
import functools

import jax
import jax.numpy as jnp
from jax import lax
from jax.experimental import pallas as pl
from jax.experimental.pallas import tpu as pltpu
from jax.sharding import PartitionSpec as P

HEADS = 16
HEAD_DIM = 128
REACH = 2
MESH = pl.DeviceIdType.MESH
PIECES = 2
DIRECT = 1
QUERY = 3
NEVER = -1e30
RELAY = 1


def kernel(
    n,
    heads,
    rows,
    q_hbm,
    k_hbm,
    v_hbm,
    seg_hbm,
    mod_hbm,
    att,
    inverse_ref,
    image_ref,
    q_own,
    own,
    buf1,
    buf2,
    hop,
    q_next,
    part_out,
    lse_out,
    part_in,
    lse_in,
    seg_ref,
    mod_ref,
    seg1,
    seg2,
    seg_next,
    bias,
    bias_next,
    squares,
    mine,
    theirs,
    own_sem,
    q_sem,
    send_a,
    send_b,
    send_c,
    recv_1,
    recv_2,
    hop_send,
    hop_recv,
    ask_sem,
    part_sem,
    lse_sem,
    id_sem,
    seg_send,
    seg_recv,
    sq_sem,
):
    s = lax.axis_index("seq")
    t = lax.axis_index("tp")
    even = lax.rem(s, 2) == 0
    odd = lax.rem(s, 2) == 1
    has_next = s + 2 < n
    has_prev = s >= 2
    ahead = odd & (s + 1 < n)
    behind = even & has_prev
    asks = even & has_prev
    answers = even & has_next
    pair = s + 1 - 2 * lax.rem(s, 2)

    half = PIECES // 2
    depth = rows // half
    last = heads - 1
    kept = heads - QUERY
    shipped = range(kept, heads)
    cuts = n // 2 - 1
    scale = HEAD_DIM ** (-0.5)

    def direct_into(block):
        return DIRECT + 0 * block

    leaving = jnp.where(ahead, direct_into(s + 1), 0)
    passing = jnp.where(even & has_next, direct_into(s + 2), 0)
    arriving = jnp.where(asks, direct_into(s), 0)
    beside = heads - jnp.where(odd & has_prev, direct_into(s - 1), 0)

    def columns_of(h):
        return pl.ds(h * HEAD_DIM, HEAD_DIM)

    def load_piece(h, p):
        source = k_hbm if p < half else v_hbm
        piece = pl.ds((p % half) * depth, depth)
        return pltpu.make_async_copy(
            source.at[piece, columns_of(h)], own.at[h, p], own_sem
        )

    def load_q(h):
        return pltpu.make_async_copy(q_hbm.at[:, columns_of(h)], q_own.at[h], q_sem)

    def load_ids(i):
        source, target = ((seg_hbm, seg_ref), (mod_hbm, mod_ref))[i]
        return pltpu.make_async_copy(source, target, id_sem.at[i])

    barrier = pltpu.get_barrier_semaphore()
    relay = t == RELAY
    passes = even & has_next & relay
    across = (odd & ~relay & (s + 1 < n)) | passes
    peers = (
        (None, {"tp": 1 - t}),
        (None, {"seq": pair}),
        (has_next, {"seq": s + 2}),
        (has_prev, {"seq": s - 2}),
        (across, {"seq": pair, "tp": 1 - t}),
        (passes, {"seq": s + 2, "tp": 1 - t}),
        (behind & ~relay, {"seq": s - 2, "tp": 1 - t}),
    )
    expected = 0
    for condition, peer in peers:

        def greet(peer=peer):
            pl.semaphore_signal(barrier, inc=1, device_id=peer, device_id_type=MESH)

        if condition is None:
            greet()
            expected = expected + 1
        else:
            pl.when(condition)(greet)
            expected = expected + jnp.where(condition, 1, 0)

    load_ids(0).start()
    for h in range(heads):
        for p in range(PIECES):
            load_piece(h, p).start()
        load_q(h).start()
    load_ids(1).start()
    for i in (0, 1):
        load_ids(i).wait()
    pltpu.make_async_copy(own, own, own_sem).wait()
    pltpu.make_async_copy(q_own, q_own, q_sem).wait()
    pl.semaphore_wait(barrier, expected)

    def remote(source, target, send, recv, where, core=t):
        return pltpu.make_async_remote_copy(
            src_ref=source,
            dst_ref=target,
            send_sem=send,
            recv_sem=recv,
            device_id={"seq": where, "tp": core},
            device_id_type=MESH,
        )

    def flow_a(h, p):
        return remote(own.at[h, p], buf1.at[h, p], send_a, recv_1.at[h, p], pair)

    def flow_b(h, p):
        return remote(own.at[h, p], buf2.at[h, p], send_b, recv_2.at[h, p], s + 2)

    def flow_c(h, p):
        return remote(buf2.at[h, p], buf1.at[h, p], send_c.at[h], recv_1.at[h, p], pair)

    def flow_d(i, p):
        return remote(
            own.at[last - i, p],
            hop.at[t, i, p],
            hop_send.at[t, i, p],
            hop_recv.at[t, i, p],
            pair,
            RELAY,
        )

    def hop_in(i, p, core):
        return remote(
            own.at[last - i, p],
            hop.at[core, i, p],
            hop_send.at[core, i, p],
            hop_recv.at[core, i, p],
            pair,
        )

    def flow_e(i, p, core):
        return remote(
            hop.at[core, i, p],
            buf1.at[last - i, p],
            hop_send.at[core, i, p],
            recv_1.at[last - i, p],
            s + 2,
            core,
        )

    def ask(i):
        return remote(
            q_own.at[kept + i], q_next.at[i], ask_sem.at[0, i], ask_sem.at[1, i], s - 2
        )

    def answer(i):
        return remote(
            part_out.at[i], part_in.at[i], part_sem.at[0, i], part_sem.at[1, i], s + 2
        )

    def answer_lse(i):
        return remote(lse_out.at[i], lse_in.at[i], lse_sem.at[0, i], lse_sem.at[1, i], s + 2)

    def forwards(h):
        return odd & has_prev & (h < beside)

    def seg_a():
        return remote(seg_ref, seg1, seg_send.at[0], seg_recv.at[0], pair)

    def seg_b():
        return remote(seg_ref, seg2, seg_send.at[1], seg_recv.at[1], s + 2)

    def seg_c():
        return remote(seg2, seg1, seg_send.at[2], seg_recv.at[0], pair)

    def seg_d():
        return remote(seg_ref, seg_next, seg_send.at[3], seg_recv.at[2], s - 2)

    @pl.when(even)
    def _():
        seg_a().start()

    @pl.when(has_next)
    def _():
        seg_b().start()

    @pl.when(asks)
    def _():
        seg_d().start()
        for i in range(QUERY):
            ask(i).start()

    for i in range(DIRECT):

        @pl.when(i < leaving)
        def _():
            for p in range(PIECES):
                flow_d(i, p).start()

    def send(h, carry):
        for p in range(PIECES):

            @pl.when(has_next & (odd | (h < kept)))
            def _():
                flow_b(h, p).start()

            @pl.when(even)
            def _():
                flow_a(h, p).start()

        return carry

    lax.fori_loop(0, heads, send, 0)

    def arrive(h, pieces):
        for p in pieces:

            @pl.when(s >= 1)
            def _():
                flow_a(h, p).wait_recv()

    def reach(h, p):
        @pl.when(has_prev)
        def _():
            flow_b(h, p).wait_recv()

        @pl.when(forwards(h))
        def _():
            flow_c(h, p).start()

    def pass_on(h):
        for p in range(PIECES):
            reach(h, p)

    @pl.when(odd & has_prev)
    def _():
        seg_b().wait_recv()
        seg_c().start()
        pass_on(0)

    @pl.when(s < 1)
    def _():
        buf1[...] = jnp.zeros_like(buf1)
        seg1[...] = jnp.full_like(seg1, -1)

    @pl.when(s < 2)
    def _():
        buf2[...] = jnp.zeros_like(buf2)
        seg2[...] = jnp.full_like(seg2, -1)
        part_in[...] = jnp.zeros_like(part_in)
        lse_in[...] = jnp.full_like(lse_in, NEVER)

    def column(row):
        return jnp.transpose(jnp.broadcast_to(row, (HEAD_DIM, rows)))

    query_seg = column(seg_ref[...])[:, :1]
    query_pos = lax.broadcasted_iota(jnp.int32, (rows, rows), 0)
    key_pos = lax.broadcasted_iota(jnp.int32, (rows, rows), 1)
    allowed = (query_seg == seg_ref[...]) & (key_pos <= query_pos)
    bias[:, :rows] = jnp.where(allowed, 0.0, -jnp.inf)
    squares[...] = jnp.zeros_like(squares)
    image_ref[...] = column(mod_ref[...])

    def scores_of(query, key):
        return scale * lax.dot_general(
            query, key, (((1,), (1,)), ((), ())), preferred_element_type=jnp.float32
        )

    def relay_head(i):
        @pl.when(passes & (i < passing))
        def _():
            for core in (0, 1):
                for p in range(PIECES):
                    hop_in(i, p, core).wait_recv()
                    flow_e(i, p, core).start()

    def attend_for(i):
        h = shipped[i]
        ask(i).wait_recv()
        key = own[h, :half].reshape(rows, HEAD_DIM)
        value = own[h, half:].reshape(rows, HEAD_DIM)
        score = scores_of(q_next[i], key) + bias_next[...]
        top = jnp.max(score, axis=1, keepdims=True)
        weight = jnp.exp(score - top)
        total = jnp.sum(weight, axis=1, keepdims=True)
        acc = jnp.dot(weight.astype(jnp.bfloat16), value, preferred_element_type=jnp.float32)
        part_out[i] = (acc * (1.0 / total)).astype(jnp.bfloat16)
        lse = jnp.broadcast_to(top + jnp.log(total), (rows, HEAD_DIM))
        lse_out[i] = jnp.transpose(lse)[:8]

    def send_answer(i):
        answer_lse(i).start()
        answer(i).start()

    @pl.when(answers)
    def _():
        seg_d().wait_recv()
        asker = column(seg_next[...])[:, :1]
        bias_next[...] = jnp.where(asker == seg_ref[...], 0.0, NEVER)
        relayed = 0
        for i in range(QUERY):
            attend_for(i)
            if i > 0:
                send_answer(i - 1)
            while relayed < DIRECT and i + 1 >= 2 * relayed + 1:
                relay_head(relayed)
                relayed += 1
        send_answer(QUERY - 1)
        for i in range(relayed, DIRECT):
            relay_head(i)

    @pl.when(asks)
    def _():
        seg_b().wait_recv()

    @pl.when(s >= 1)
    def _():
        seg_a().wait_recv()

    bias[:, rows : 2 * rows] = jnp.where(query_seg == seg1[...], 0.0, -jnp.inf)
    bias[:, 2 * rows :] = jnp.where(query_seg == seg2[...], 0.0, -jnp.inf)

    def scores_with(h, block, i):
        key = block[h, :half].reshape(rows, HEAD_DIM)
        return scores_of(q_own[h], key) + bias[:, i * rows : (i + 1) * rows]

    def product(weight, value):
        return jnp.dot(weight.astype(jnp.bfloat16), value, preferred_element_type=jnp.float32)

    def values_of(block, h):
        return block[h, half:].reshape(rows, HEAD_DIM)

    def finish(h, acc, total):
        attended = (acc * (1.0 / total)).astype(jnp.bfloat16)
        att[h] = attended
        wide = attended.astype(jnp.float32)
        return wide * wide

    def head(h, pieces_apart):
        @pl.when(even)
        def _():
            for p in range(half):
                reach(h, p)

        near = scores_with(h, own, 0)
        far = scores_with(h, buf2, 2)
        arrive(h, range(half))
        middle = scores_with(h, buf1, 1)
        top = jnp.max(jnp.maximum(jnp.maximum(near, middle), far), axis=1, keepdims=True)
        near = jnp.exp(near - top)
        far = jnp.exp(far - top)
        middle = jnp.exp(middle - top)
        total = jnp.sum(near + middle + far, axis=1, keepdims=True)
        acc = product(near, values_of(own, h))

        @pl.when(even)
        def _():
            for p in range(half, PIECES):
                reach(h, p)

        if pieces_apart:
            acc = acc + product(far, values_of(buf2, h))
            for p in range(half, PIECES):
                arrive(h, (p,))
                part = middle[:, (p - half) * depth : (p - half + 1) * depth]
                acc = acc + product(part, buf1[h, p])
        else:
            arrive(h, range(half, PIECES))
            acc = acc + product(far, values_of(buf2, h)) + product(middle, values_of(buf1, h))
        return finish(h, acc, total)

    def merged(i):
        h = kept + i
        near = scores_with(h, own, 0)

        @pl.when(asks)
        def _():
            answer_lse(i).wait_recv()
            answer(i).wait_recv()

        lse = column(lse_in[i, :1])[:, :1]
        first_top = jnp.maximum(jnp.max(near, axis=1, keepdims=True), lse)
        near = jnp.exp(near - first_top)
        far = jnp.exp(lse - first_top)
        first_total = jnp.sum(near, axis=1, keepdims=True) + far
        acc = product(near, values_of(own, h)) + far * part_in[i].astype(jnp.float32)
        arrive(h, range(half))
        middle = scores_with(h, buf1, 1)
        top = jnp.maximum(jnp.max(middle, axis=1, keepdims=True), first_top)
        middle = jnp.exp(middle - top)
        again = jnp.exp(first_top - top)
        total = jnp.sum(middle, axis=1, keepdims=True) + again * first_total
        acc = acc * again
        arrive(h, range(half, PIECES))
        acc = acc + product(middle, values_of(buf1, h))
        return finish(h, acc, total)

    def one(h, carry):
        @pl.when(odd & (h + 1 < beside))
        def _():
            pass_on(h + 1)

        @pl.when(odd & (h >= beside))
        def _():
            pass_on(h)

        squares[...] += head(h, False)
        return carry

    def conclude(wide):
        partial = jnp.sum(squares[...] + wide, axis=1, keepdims=True)
        mine[...] = jnp.broadcast_to(partial, mine.shape)

    lax.fori_loop(0, jnp.where(odd, last, kept), one, 0)

    @pl.when(odd & has_prev & (beside < heads))
    def _():
        pass_on(last)

    @pl.when(odd)
    def _():
        conclude(head(last, True))

    def shipped_at(j):
        waiting = QUERY - 1 - arriving
        early = jnp.where(j < waiting, j, QUERY - 1 - (j - waiting))
        return jnp.where(j == QUERY - 1, waiting, early)

    def joined(j, carry):
        squares[...] += merged(shipped_at(j))
        return carry

    @pl.when(even)
    def _():
        lax.fori_loop(0, QUERY - 1, joined, 0)
        conclude(merged(shipped_at(QUERY - 1)))

    swap = pltpu.make_async_remote_copy(
        src_ref=mine,
        dst_ref=theirs,
        send_sem=sq_sem.at[0],
        recv_sem=sq_sem.at[1],
        device_id={"tp": 1 - t},
        device_id_type=MESH,
    )
    swap.start()

    def sent(ref, send):
        remote(ref, ref, send, recv_1.at[0, 0], pair).wait_send()

    for i in range(DIRECT):

        @pl.when(i < leaving)
        def _():
            for p in range(PIECES):
                flow_d(i, p).wait_send()

        @pl.when(passes & (i < passing))
        def _():
            for core in (0, 1):
                for p in range(PIECES):
                    flow_e(i, p, core).wait_send()

    @pl.when(asks)
    def _():
        seg_d().wait_send()
        for i in range(QUERY):
            ask(i).wait_send()

    @pl.when(answers)
    def _():
        for i in range(QUERY):
            answer(i).wait_send()
            answer_lse(i).wait_send()

    @pl.when(even)
    def _():
        seg_a().wait_send()
        sent(own, send_a)

    @pl.when(has_next)
    def _():
        seg_b().wait_send()
        sent(own.at[:kept], send_b)

    @pl.when(odd & has_next)
    def _():
        sent(own.at[kept:], send_b)

    @pl.when(odd & has_prev)
    def _():
        seg_c().wait_send()

    for h in range(heads):

        @pl.when(forwards(h))
        def _():
            sent(buf2.at[h], send_c.at[h])

    swap.wait_recv()
    mean_square = (mine[...] + theirs[...]) / (HEADS * HEAD_DIM)
    inverse_ref[...] = lax.rsqrt(mean_square + 1e-05)
    swap.wait_send()


def blend(heads, att, inverse_ref, image_ref, gain_ref, out_hbm, staged, out_sem):
    inverse = inverse_ref[...]
    image = image_ref[...] == 1
    copies = []
    for h in range(heads):
        columns = slice(h * HEAD_DIM, (h + 1) * HEAD_DIM)
        gain = jnp.where(image, gain_ref[1:2, columns], gain_ref[0:1, columns])
        staged[h] = (att[h].astype(jnp.float32) * inverse * gain).astype(staged.dtype)
        copy = pltpu.make_async_copy(
            staged.at[h], out_hbm.at[:, pl.ds(h * HEAD_DIM, HEAD_DIM)], out_sem.at[h]
        )
        copy.start()
        copies.append(copy)
    for copy in copies:
        copy.wait()


def on_device(n, queries, keys, values, segment_ids, modality, norm_gain):
    rows, width = queries.shape
    heads = width // HEAD_DIM
    vmem = pl.BlockSpec(memory_space=pltpu.VMEM)
    hbm = pl.BlockSpec(memory_space=pltpu.HBM)
    depth = 2 * rows // PIECES
    block = pltpu.VMEM((heads, PIECES, depth, HEAD_DIM), jnp.bfloat16)
    asked = pltpu.VMEM((QUERY, rows, HEAD_DIM), jnp.bfloat16)
    ids = pltpu.VMEM((1, rows), jnp.int32)
    flow = pltpu.SemaphoreType.DMA((heads, PIECES))
    att, inverse, image = pl.pallas_call(
        functools.partial(kernel, n, heads, rows),
        out_shape=(
            pltpu.VMEM((heads, rows, HEAD_DIM), jnp.bfloat16),
            pltpu.VMEM((rows, HEAD_DIM), jnp.float32),
            pltpu.VMEM((rows, HEAD_DIM), jnp.int32),
        ),
        in_specs=[hbm, hbm, hbm, hbm, hbm],
        out_specs=(vmem, vmem, vmem),
        scratch_shapes=[
            pltpu.VMEM((heads, rows, HEAD_DIM), jnp.bfloat16),
            block,
            block,
            block,
            pltpu.VMEM((2, DIRECT, PIECES, depth, HEAD_DIM), jnp.bfloat16),
            asked,
            asked,
            pltpu.VMEM((QUERY, 8, rows), jnp.float32),
            asked,
            pltpu.VMEM((QUERY, 8, rows), jnp.float32),
            ids,
            ids,
            ids,
            ids,
            ids,
            pltpu.VMEM((rows, (REACH + 1) * rows), jnp.float32),
            pltpu.VMEM((rows, rows), jnp.float32),
            pltpu.VMEM((rows, HEAD_DIM), jnp.float32),
            pltpu.VMEM((rows, HEAD_DIM), jnp.float32),
            pltpu.VMEM((rows, HEAD_DIM), jnp.float32),
            pltpu.SemaphoreType.DMA,
            pltpu.SemaphoreType.DMA,
            pltpu.SemaphoreType.DMA,
            pltpu.SemaphoreType.DMA,
            pltpu.SemaphoreType.DMA((heads,)),
            flow,
            flow,
            pltpu.SemaphoreType.DMA((2, DIRECT, PIECES)),
            pltpu.SemaphoreType.DMA((2, DIRECT, PIECES)),
            pltpu.SemaphoreType.DMA((2, QUERY)),
            pltpu.SemaphoreType.DMA((2, QUERY)),
            pltpu.SemaphoreType.DMA((2, QUERY)),
            pltpu.SemaphoreType.DMA((2,)),
            pltpu.SemaphoreType.DMA((4,)),
            pltpu.SemaphoreType.DMA((3,)),
            pltpu.SemaphoreType.DMA((2,)),
        ],
        compiler_params=pltpu.CompilerParams(
            collective_id=0, has_side_effects=True
        ),
    )(queries, keys, values, segment_ids.reshape(1, rows), modality.reshape(1, rows))
    return pl.pallas_call(
        functools.partial(blend, heads),
        out_shape=jax.ShapeDtypeStruct((rows, width), jnp.bfloat16),
        in_specs=[vmem, vmem, vmem, vmem],
        out_specs=hbm,
        scratch_shapes=[
            pltpu.VMEM((heads, rows, HEAD_DIM), jnp.bfloat16),
            pltpu.SemaphoreType.DMA((heads,)),
        ],
        compiler_params=pltpu.CompilerParams(vmem_limit_bytes=8 * 2**20),
    )(att, inverse, image, norm_gain)


def solution(mesh):
    return jax.shard_map(
        functools.partial(on_device, mesh.shape["seq"]),
        mesh=mesh,
        in_specs=(
            P(("grp", "seq"), "tp"),
            P(("grp", "seq"), "tp"),
            P(("grp", "seq"), "tp"),
            P(("grp", "seq")),
            P(("grp", "seq")),
            P(None, "tp"),
        ),
        out_specs=P(("grp", "seq"), "tp"),
        check_vma=False,
    )
```

```python
import functools

import jax
import jax.numpy as jnp
from jax import lax
from jax.experimental import pallas as pl
from jax.experimental.pallas import tpu as pltpu
from jax.sharding import PartitionSpec as P

HEADS = 16
HEAD_DIM = 128
REACH = 2
MESH = pl.DeviceIdType.MESH
PIECES = 2
DIRECT = 2
FEWEST = 2
NEVER = -1e30


def kernel(
    n,
    heads,
    rows,
    q_hbm,
    k_hbm,
    v_hbm,
    seg_hbm,
    mod_hbm,
    att,
    inverse_ref,
    image_ref,
    q_own,
    own,
    buf1,
    buf2,
    hop,
    q_next,
    part_out,
    lse_out,
    part_in,
    lse_in,
    seg_ref,
    mod_ref,
    seg1,
    seg2,
    seg_next,
    bias,
    bias_next,
    squares,
    mine,
    theirs,
    own_sem,
    q_sem,
    send_a,
    send_b,
    send_c,
    recv_1,
    recv_2,
    hop_send,
    hop_recv,
    ask_sem,
    part_sem,
    lse_sem,
    id_sem,
    seg_send,
    seg_recv,
    sq_sem,
):
    s = lax.axis_index("seq")
    t = lax.axis_index("tp")
    even = lax.rem(s, 2) == 0
    odd = lax.rem(s, 2) == 1
    has_next = s + 2 < n
    has_prev = s >= 2
    ahead = odd & (s + 1 < n)
    behind = even & has_prev
    asks = even & has_prev
    answers = even & has_next
    pair = s + 1 - 2 * lax.rem(s, 2)

    half = PIECES // 2
    depth = rows // half
    last = heads - 1
    cuts = n // 2 - 1
    scale = HEAD_DIM ** (-0.5)

    def direct_into(block):
        return FEWEST + ((cuts - block // 2) * (DIRECT - FEWEST)) // max(cuts - 1, 1)

    leaving = jnp.where(ahead, direct_into(s + 1), 0)
    passing = jnp.where(even & has_next, direct_into(s + 2), 0)
    arriving = jnp.where(asks, direct_into(s), 0)
    beside = heads - jnp.where(odd & has_prev, direct_into(s - 1), 0)

    def turn(j, direct):
        mixed = jnp.where(lax.rem(j, 2) == 0, last - j // 2, j // 2)
        return jnp.where(j < 2 * direct, mixed, j - direct)

    def columns_of(h):
        return pl.ds(h * HEAD_DIM, HEAD_DIM)

    def load_piece(h, p):
        source = k_hbm if p < half else v_hbm
        piece = pl.ds((p % half) * depth, depth)
        return pltpu.make_async_copy(
            source.at[piece, columns_of(h)], own.at[h, p], own_sem
        )

    def load_q(h):
        return pltpu.make_async_copy(q_hbm.at[:, columns_of(h)], q_own.at[h], q_sem)

    def load_ids(i):
        source, target = ((seg_hbm, seg_ref), (mod_hbm, mod_ref))[i]
        return pltpu.make_async_copy(source, target, id_sem.at[i])

    barrier = pltpu.get_barrier_semaphore()
    peers = (
        (None, {"tp": 1 - t}),
        (None, {"seq": pair}),
        (has_next, {"seq": s + 2}),
        (has_prev, {"seq": s - 2}),
    )
    expected = 0
    for condition, peer in peers:

        def greet(peer=peer):
            pl.semaphore_signal(barrier, inc=1, device_id=peer, device_id_type=MESH)

        if condition is None:
            greet()
            expected = expected + 1
        else:
            pl.when(condition)(greet)
            expected = expected + jnp.where(condition, 1, 0)

    load_ids(0).start()
    for h in range(heads):
        for p in range(PIECES):
            load_piece(h, p).start()
        load_q(h).start()
    load_ids(1).start()
    for i in (0, 1):
        load_ids(i).wait()
    pltpu.make_async_copy(own, own, own_sem).wait()
    pltpu.make_async_copy(q_own, q_own, q_sem).wait()
    pl.semaphore_wait(barrier, expected)

    def remote(source, target, send, recv, where):
        return pltpu.make_async_remote_copy(
            src_ref=source,
            dst_ref=target,
            send_sem=send,
            recv_sem=recv,
            device_id={"seq": where},
            device_id_type=MESH,
        )

    def flow_a(h, p):
        return remote(own.at[h, p], buf1.at[h, p], send_a, recv_1.at[h, p], pair)

    def flow_b(h, p):
        return remote(own.at[h, p], buf2.at[h, p], send_b, recv_2.at[h, p], s + 2)

    def flow_c(h, p):
        return remote(buf2.at[h, p], buf1.at[h, p], send_c.at[h], recv_1.at[h, p], pair)

    def flow_d(i, p):
        return remote(
            own.at[last - i, p], hop.at[i, p], hop_send.at[i, p], hop_recv.at[i, p], pair
        )

    def flow_e(i, p):
        return remote(
            hop.at[i, p], buf1.at[last - i, p], hop_send.at[i, p], recv_1.at[last - i, p], s + 2
        )

    def ask(i):
        return remote(
            q_own.at[i], q_next.at[i], ask_sem.at[0, i], ask_sem.at[1, i], s - 2
        )

    def answer(i):
        return remote(
            part_out.at[i], part_in.at[i], part_sem.at[0, i], part_sem.at[1, i], s + 2
        )

    def answer_lse(i):
        return remote(lse_out.at[i], lse_in.at[i], lse_sem.at[0, i], lse_sem.at[1, i], s + 2)

    def forwards(h):
        return odd & has_prev & (h < beside)

    def seg_a():
        return remote(seg_ref, seg1, seg_send.at[0], seg_recv.at[0], pair)

    def seg_b():
        return remote(seg_ref, seg2, seg_send.at[1], seg_recv.at[1], s + 2)

    def seg_c():
        return remote(seg2, seg1, seg_send.at[2], seg_recv.at[0], pair)

    def seg_d():
        return remote(seg_ref, seg_next, seg_send.at[3], seg_recv.at[2], s - 2)

    @pl.when(even)
    def _():
        seg_a().start()

    @pl.when(odd & has_next)
    def _():
        seg_b().start()

    @pl.when(asks)
    def _():
        seg_d().start()

        def send_ask(j, carry):
            ask(turn(j, arriving)).start()
            return carry

        lax.fori_loop(0, heads, send_ask, 0)

    for i in range(DIRECT):

        @pl.when(i < leaving)
        def _():
            for p in range(PIECES):
                flow_d(i, p).start()

    def send(h, carry):
        for p in range(PIECES):

            @pl.when(odd & has_next)
            def _():
                flow_b(h, p).start()

            @pl.when(even)
            def _():
                flow_a(h, p).start()

        return carry

    lax.fori_loop(0, heads, send, 0)

    def arrive(h, pieces):
        for p in pieces:

            @pl.when(s >= 1)
            def _():
                flow_a(h, p).wait_recv()

    def reach(h, p):
        @pl.when(odd & has_prev)
        def _():
            flow_b(h, p).wait_recv()

        @pl.when(forwards(h))
        def _():
            flow_c(h, p).start()

    def pass_on(h):
        for p in range(PIECES):
            reach(h, p)

    @pl.when(odd & has_prev)
    def _():
        seg_b().wait_recv()
        seg_c().start()
        pass_on(0)

    @pl.when(s < 1)
    def _():
        buf1[...] = jnp.zeros_like(buf1)
        seg1[...] = jnp.full_like(seg1, -1)

    @pl.when(s < 2)
    def _():
        buf2[...] = jnp.zeros_like(buf2)
        seg2[...] = jnp.full_like(seg2, -1)
        part_in[...] = jnp.zeros_like(part_in)
        lse_in[...] = jnp.full_like(lse_in, NEVER)

    def column(row):
        return jnp.transpose(jnp.broadcast_to(row, (HEAD_DIM, rows)))

    query_seg = column(seg_ref[...])[:, :1]
    query_pos = lax.broadcasted_iota(jnp.int32, (rows, rows), 0)
    key_pos = lax.broadcasted_iota(jnp.int32, (rows, rows), 1)
    allowed = (query_seg == seg_ref[...]) & (key_pos <= query_pos)
    bias[:, :rows] = jnp.where(allowed, 0.0, -jnp.inf)
    squares[...] = jnp.zeros_like(squares)
    image_ref[...] = column(mod_ref[...])

    def scores_of(query, key):
        return scale * lax.dot_general(
            query, key, (((1,), (1,)), ((), ())), preferred_element_type=jnp.float32
        )

    def relay_head(i):
        for p in range(PIECES):
            flow_d(i, p).wait_recv()
            flow_e(i, p).start()

    def attend_for(i):
        ask(i).wait_recv()
        key = own[i, :half].reshape(rows, HEAD_DIM)
        value = own[i, half:].reshape(rows, HEAD_DIM)
        score = scores_of(q_next[i], key) + bias_next[...]
        top = jnp.max(score, axis=1, keepdims=True)
        weight = jnp.exp(score - top)
        total = jnp.sum(weight, axis=1, keepdims=True)
        acc = jnp.dot(weight.astype(jnp.bfloat16), value, preferred_element_type=jnp.float32)
        part_out[i] = (acc * (1.0 / total)).astype(jnp.bfloat16)
        lse = jnp.broadcast_to(top + jnp.log(total), (rows, HEAD_DIM))
        lse_out[i] = jnp.transpose(lse)[:8]

    def send_answer(i):
        answer_lse(i).start()
        answer(i).start()

    @pl.when(answers)
    def _():
        seg_d().wait_recv()
        asker = column(seg_next[...])[:, :1]
        bias_next[...] = jnp.where(asker == seg_ref[...], 0.0, NEVER)

        def attend_next(j, carry):
            h = turn(j, passing)
            attend_for(h)

            @pl.when(j > 0)
            def _():
                send_answer(turn(j - 1, passing))

            @pl.when((lax.rem(j, 2) == 0) & (j < 2 * passing))
            def _():
                relay_head(j // 2)

            return carry

        lax.fori_loop(0, heads, attend_next, 0)
        send_answer(turn(last, passing))

    @pl.when(s >= 1)
    def _():
        seg_a().wait_recv()

    bias[:, rows : 2 * rows] = jnp.where(query_seg == seg1[...], 0.0, -jnp.inf)
    bias[:, 2 * rows :] = jnp.where(query_seg == seg2[...], 0.0, -jnp.inf)

    def scores_with(h, block, i):
        key = block[h, :half].reshape(rows, HEAD_DIM)
        return scores_of(q_own[h], key) + bias[:, i * rows : (i + 1) * rows]

    def product(weight, value):
        return jnp.dot(weight.astype(jnp.bfloat16), value, preferred_element_type=jnp.float32)

    def values_of(block, h):
        return block[h, half:].reshape(rows, HEAD_DIM)

    def finish(h, acc, total):
        attended = (acc * (1.0 / total)).astype(jnp.bfloat16)
        att[h] = attended
        wide = attended.astype(jnp.float32)
        return wide * wide

    def head(h, pieces_apart):
        near = scores_with(h, own, 0)
        far = scores_with(h, buf2, 2)
        arrive(h, range(half))
        middle = scores_with(h, buf1, 1)
        top = jnp.max(jnp.maximum(jnp.maximum(near, middle), far), axis=1, keepdims=True)
        near = jnp.exp(near - top)
        far = jnp.exp(far - top)
        middle = jnp.exp(middle - top)
        total = jnp.sum(near + middle + far, axis=1, keepdims=True)
        acc = product(near, values_of(own, h))

        if pieces_apart:
            acc = acc + product(far, values_of(buf2, h))
            for p in range(half, PIECES):
                arrive(h, (p,))
                part = middle[:, (p - half) * depth : (p - half + 1) * depth]
                acc = acc + product(part, buf1[h, p])
        else:
            arrive(h, range(half, PIECES))
            acc = acc + product(far, values_of(buf2, h)) + product(middle, values_of(buf1, h))
        return finish(h, acc, total)

    def merged(h, apart):
        near = scores_with(h, own, 0)

        @pl.when(asks)
        def _():
            answer_lse(h).wait_recv()
            answer(h).wait_recv()

        lse = column(lse_in[h, :1])[:, :1]
        if not apart:
            arrive(h, range(half))
            middle = scores_with(h, buf1, 1)
            top = jnp.max(jnp.maximum(near, middle), axis=1, keepdims=True)
            top = jnp.maximum(top, lse)
            near = jnp.exp(near - top)
            middle = jnp.exp(middle - top)
            far = jnp.exp(lse - top)
            total = jnp.sum(near + middle, axis=1, keepdims=True) + far
            acc = product(near, values_of(own, h)) + far * part_in[h].astype(jnp.float32)
            arrive(h, range(half, PIECES))
            return finish(h, acc + product(middle, values_of(buf1, h)), total)
        first_top = jnp.maximum(jnp.max(near, axis=1, keepdims=True), lse)
        near = jnp.exp(near - first_top)
        far = jnp.exp(lse - first_top)
        first_total = jnp.sum(near, axis=1, keepdims=True) + far
        acc = product(near, values_of(own, h)) + far * part_in[h].astype(jnp.float32)
        arrive(h, range(half))
        middle = scores_with(h, buf1, 1)
        top = jnp.maximum(jnp.max(middle, axis=1, keepdims=True), first_top)
        middle = jnp.exp(middle - top)
        again = jnp.exp(first_top - top)
        total = jnp.sum(middle, axis=1, keepdims=True) + again * first_total
        acc = acc * again
        arrive(h, range(half, PIECES))
        return finish(h, acc + product(middle, values_of(buf1, h)), total)

    def one(h, carry):
        @pl.when(h + 1 < beside)
        def _():
            pass_on(h + 1)

        @pl.when(h >= beside)
        def _():
            pass_on(h)

        squares[...] += head(h, False)
        return carry

    def conclude(wide):
        partial = jnp.sum(squares[...] + wide, axis=1, keepdims=True)
        mine[...] = jnp.broadcast_to(partial, mine.shape)

    @pl.when(odd)
    def _():
        lax.fori_loop(0, last, one, 0)

        @pl.when(beside < heads)
        def _():
            pass_on(last)

        conclude(head(last, True))

    def joined(j, carry):
        squares[...] += merged(turn(j, arriving), False)
        return carry

    @pl.when(even)
    def _():
        lax.fori_loop(0, last, joined, 0)
        conclude(merged(turn(last, arriving), True))

    swap = pltpu.make_async_remote_copy(
        src_ref=mine,
        dst_ref=theirs,
        send_sem=sq_sem.at[0],
        recv_sem=sq_sem.at[1],
        device_id={"tp": 1 - t},
        device_id_type=MESH,
    )
    swap.start()

    def sent(ref, send):
        remote(ref, ref, send, recv_1.at[0, 0], pair).wait_send()

    for i in range(DIRECT):

        @pl.when(i < leaving)
        def _():
            for p in range(PIECES):
                flow_d(i, p).wait_send()

        @pl.when(i < passing)
        def _():
            for p in range(PIECES):
                flow_e(i, p).wait_send()

    @pl.when(asks)
    def _():
        seg_d().wait_send()
        for i in range(heads):
            ask(i).wait_send()

    @pl.when(answers)
    def _():
        for i in range(heads):
            answer(i).wait_send()
            answer_lse(i).wait_send()

    @pl.when(even)
    def _():
        seg_a().wait_send()
        sent(own, send_a)

    @pl.when(odd & has_next)
    def _():
        seg_b().wait_send()
        sent(own, send_b)

    @pl.when(odd & has_prev)
    def _():
        seg_c().wait_send()

    for h in range(heads):

        @pl.when(forwards(h))
        def _():
            sent(buf2.at[h], send_c.at[h])

    swap.wait_recv()
    mean_square = (mine[...] + theirs[...]) / (HEADS * HEAD_DIM)
    inverse_ref[...] = lax.rsqrt(mean_square + 1e-05)
    swap.wait_send()


def blend(heads, att, inverse_ref, image_ref, gain_ref, out_hbm, staged, out_sem):
    inverse = inverse_ref[...]
    image = image_ref[...] == 1
    copies = []
    for h in range(heads):
        columns = slice(h * HEAD_DIM, (h + 1) * HEAD_DIM)
        gain = jnp.where(image, gain_ref[1:2, columns], gain_ref[0:1, columns])
        staged[h] = (att[h].astype(jnp.float32) * inverse * gain).astype(staged.dtype)
        copy = pltpu.make_async_copy(
            staged.at[h], out_hbm.at[:, pl.ds(h * HEAD_DIM, HEAD_DIM)], out_sem.at[h]
        )
        copy.start()
        copies.append(copy)
    for copy in copies:
        copy.wait()


def on_device(n, queries, keys, values, segment_ids, modality, norm_gain):
    rows, width = queries.shape
    heads = width // HEAD_DIM
    vmem = pl.BlockSpec(memory_space=pltpu.VMEM)
    hbm = pl.BlockSpec(memory_space=pltpu.HBM)
    depth = 2 * rows // PIECES
    block = pltpu.VMEM((heads, PIECES, depth, HEAD_DIM), jnp.bfloat16)
    asked = pltpu.VMEM((heads, rows, HEAD_DIM), jnp.bfloat16)
    ids = pltpu.VMEM((1, rows), jnp.int32)
    flow = pltpu.SemaphoreType.DMA((heads, PIECES))
    att, inverse, image = pl.pallas_call(
        functools.partial(kernel, n, heads, rows),
        out_shape=(
            pltpu.VMEM((heads, rows, HEAD_DIM), jnp.bfloat16),
            pltpu.VMEM((rows, HEAD_DIM), jnp.float32),
            pltpu.VMEM((rows, HEAD_DIM), jnp.int32),
        ),
        in_specs=[hbm, hbm, hbm, hbm, hbm],
        out_specs=(vmem, vmem, vmem),
        scratch_shapes=[
            pltpu.VMEM((heads, rows, HEAD_DIM), jnp.bfloat16),
            block,
            block,
            block,
            pltpu.VMEM((DIRECT, PIECES, depth, HEAD_DIM), jnp.bfloat16),
            asked,
            asked,
            pltpu.VMEM((heads, 8, rows), jnp.float32),
            asked,
            pltpu.VMEM((heads, 8, rows), jnp.float32),
            ids,
            ids,
            ids,
            ids,
            ids,
            pltpu.VMEM((rows, (REACH + 1) * rows), jnp.float32),
            pltpu.VMEM((rows, rows), jnp.float32),
            pltpu.VMEM((rows, HEAD_DIM), jnp.float32),
            pltpu.VMEM((rows, HEAD_DIM), jnp.float32),
            pltpu.VMEM((rows, HEAD_DIM), jnp.float32),
            pltpu.SemaphoreType.DMA,
            pltpu.SemaphoreType.DMA,
            pltpu.SemaphoreType.DMA,
            pltpu.SemaphoreType.DMA,
            pltpu.SemaphoreType.DMA((heads,)),
            flow,
            flow,
            pltpu.SemaphoreType.DMA((DIRECT, PIECES)),
            pltpu.SemaphoreType.DMA((DIRECT, PIECES)),
            pltpu.SemaphoreType.DMA((2, heads)),
            pltpu.SemaphoreType.DMA((2, heads)),
            pltpu.SemaphoreType.DMA((2, heads)),
            pltpu.SemaphoreType.DMA((2,)),
            pltpu.SemaphoreType.DMA((4,)),
            pltpu.SemaphoreType.DMA((3,)),
            pltpu.SemaphoreType.DMA((2,)),
        ],
        compiler_params=pltpu.CompilerParams(
            collective_id=0, has_side_effects=True
        ),
    )(queries, keys, values, segment_ids.reshape(1, rows), modality.reshape(1, rows))
    return pl.pallas_call(
        functools.partial(blend, heads),
        out_shape=jax.ShapeDtypeStruct((rows, width), jnp.bfloat16),
        in_specs=[vmem, vmem, vmem, vmem],
        out_specs=hbm,
        scratch_shapes=[
            pltpu.VMEM((heads, rows, HEAD_DIM), jnp.bfloat16),
            pltpu.SemaphoreType.DMA((heads,)),
        ],
        compiler_params=pltpu.CompilerParams(vmem_limit_bytes=8 * 2**20),
    )(att, inverse, image, norm_gain)


def solution(mesh):
    return jax.shard_map(
        functools.partial(on_device, mesh.shape["seq"]),
        mesh=mesh,
        in_specs=(
            P(("grp", "seq"), "tp"),
            P(("grp", "seq"), "tp"),
            P(("grp", "seq"), "tp"),
            P(("grp", "seq")),
            P(("grp", "seq")),
            P(None, "tp"),
        ),
        out_specs=P(("grp", "seq"), "tp"),
        check_vma=False,
    )
```

```python
import functools

import jax
import jax.numpy as jnp
from jax import lax
from jax.experimental import pallas as pl
from jax.experimental.pallas import tpu as pltpu
from jax.sharding import PartitionSpec as P

HEADS = 16
HEAD_DIM = 128
REACH = 2
MESH = pl.DeviceIdType.MESH
PIECES = 2
MOST = (4, 6)
LEAST = (4, 2)
NEVER = -1e30
KEPT = 2
SHIPPER = 0


def kernel(
    n,
    heads,
    rows,
    q_hbm,
    k_hbm,
    v_hbm,
    seg_hbm,
    mod_hbm,
    att,
    inverse_ref,
    image_ref,
    q_own,
    own,
    buf1,
    buf2,
    hop,
    q_next,
    part_out,
    lse_out,
    part_in,
    lse_in,
    seg_ref,
    mod_ref,
    seg1,
    seg2,
    seg_next,
    seg_beside,
    bias,
    bias_next,
    squares,
    mine,
    theirs,
    own_sem,
    q_sem,
    send_a,
    send_b,
    send_c,
    recv_1,
    recv_2,
    hop_send,
    hop_recv,
    ask_sem,
    part_sem,
    lse_sem,
    id_sem,
    seg_send,
    seg_recv,
    sq_sem,
):
    s = lax.axis_index("seq")
    t = lax.axis_index("tp")
    even = lax.rem(s, 2) == 0
    odd = lax.rem(s, 2) == 1
    has_next = s + 2 < n
    has_prev = s >= 2
    ahead = odd & (s + 1 < n)
    behind = even & has_prev
    asks = even & has_prev
    answers = even & has_next
    pair = s + 1 - 2 * lax.rem(s, 2)
    ships = odd & (t == SHIPPER)
    serves = even & (t == SHIPPER)
    keeps = t != SHIPPER

    half = PIECES // 2
    depth = rows // half
    last = heads - 1
    turns = heads - KEPT
    cuts = n // 2 - 1
    scale = HEAD_DIM ** (-0.5)

    def direct_into(block):
        top = jnp.where(t == 0, MOST[0], MOST[1])
        low = jnp.where(t == 0, LEAST[0], LEAST[1])
        return low + ((cuts - block // 2) * (top - low)) // max(cuts - 1, 1)

    deepest = (max(MOST + LEAST) + PIECES - 1) // PIECES
    leaving = jnp.where(ahead, direct_into(s + 1), 0)
    passing = jnp.where(even & has_next, direct_into(s + 2), 0)
    arriving = jnp.where(asks, direct_into(s), 0)
    skipped = jnp.where(odd & has_prev, direct_into(s - 1), 0)
    beside = heads - skipped // PIECES

    def unit(i, p):
        return PIECES * i + PIECES - 1 - p

    def turn(j, direct):
        mixed = jnp.where(lax.rem(j, 2) == 0, last - j // 2, KEPT + j // 2)
        return jnp.where(j < 2 * (direct // PIECES), mixed, KEPT + j - direct // PIECES)

    def columns_of(h):
        return pl.ds(h * HEAD_DIM, HEAD_DIM)

    def load_piece(h, p):
        source = k_hbm if p < half else v_hbm
        piece = pl.ds((p % half) * depth, depth)
        return pltpu.make_async_copy(
            source.at[piece, columns_of(h)], own.at[h, p], own_sem
        )

    def load_q(h):
        return pltpu.make_async_copy(q_hbm.at[:, columns_of(h)], q_own.at[h], q_sem)

    def load_ids(i):
        source, target = ((seg_hbm, seg_ref), (mod_hbm, mod_ref))[i]
        return pltpu.make_async_copy(source, target, id_sem.at[i])

    barrier = pltpu.get_barrier_semaphore()
    peers = (
        (None, {"tp": 1 - t}),
        (None, {"seq": pair}),
        (has_next, {"seq": s + 2}),
        (has_prev, {"seq": s - 2}),
    )
    expected = 0
    for condition, peer in peers:

        def greet(peer=peer):
            pl.semaphore_signal(barrier, inc=1, device_id=peer, device_id_type=MESH)

        if condition is None:
            greet()
            expected = expected + 1
        else:
            pl.when(condition)(greet)
            expected = expected + jnp.where(condition, 1, 0)

    load_ids(0).start()
    for h in range(heads):
        for p in range(PIECES):
            load_piece(h, p).start()
        load_q(h).start()
    load_ids(1).start()
    for i in (0, 1):
        load_ids(i).wait()
    pltpu.make_async_copy(own, own, own_sem).wait()
    pltpu.make_async_copy(q_own, q_own, q_sem).wait()
    pl.semaphore_wait(barrier, expected)

    def remote(source, target, send, recv, where):
        return pltpu.make_async_remote_copy(
            src_ref=source,
            dst_ref=target,
            send_sem=send,
            recv_sem=recv,
            device_id={"seq": where},
            device_id_type=MESH,
        )

    def flow_a(h, p):
        return remote(own.at[h, p], buf1.at[h, p], send_a, recv_1.at[h, p], pair)

    def flow_b(h, p):
        return remote(own.at[h, p], buf2.at[h, p], send_b, recv_2.at[h, p], s + 2)

    def flow_c(h, p):
        return remote(buf2.at[h, p], buf1.at[h, p], send_c.at[h, p], recv_1.at[h, p], pair)

    def flow_d(i, p):
        return remote(
            own.at[last - i, p], hop.at[i, p], hop_send.at[i, p], hop_recv.at[i, p], pair
        )

    def flow_e(i, p):
        return remote(
            hop.at[i, p], buf1.at[last - i, p], hop_send.at[i, p], recv_1.at[last - i, p], s + 2
        )

    def ask(i):
        return remote(
            q_own.at[i], q_next.at[i], ask_sem.at[0, i], ask_sem.at[1, i], s - 2
        )

    def answer(i):
        return remote(
            part_out.at[i], part_in.at[i], part_sem.at[0, i], part_sem.at[1, i], s + 2
        )

    def ask_beside():
        return remote(q_own.at[last], q_next.at[0], ask_sem.at[0, 0], ask_sem.at[1, 0], pair)

    def answer_beside():
        return remote(part_out.at[0], part_in.at[0], part_sem.at[0, 0], part_sem.at[1, 0], pair)

    def answer_beside_lse():
        return remote(lse_out.at[0], lse_in.at[0], lse_sem.at[0, 0], lse_sem.at[1, 0], pair)

    def answer_lse(i):
        return remote(lse_out.at[i], lse_in.at[i], lse_sem.at[0, i], lse_sem.at[1, i], s + 2)

    def forwards(h, p):
        return odd & has_prev & (unit(last - h, p) >= skipped)

    def seg_a():
        return remote(seg_ref, seg1, seg_send.at[0], seg_recv.at[0], pair)

    def seg_b():
        return remote(seg_ref, seg2, seg_send.at[1], seg_recv.at[1], s + 2)

    def seg_c():
        return remote(seg2, seg1, seg_send.at[2], seg_recv.at[0], pair)

    def seg_e():
        return remote(seg_ref, seg_beside, seg_send.at[4], seg_recv.at[3], pair)

    def seg_d():
        return remote(seg_ref, seg_next, seg_send.at[3], seg_recv.at[2], s - 2)

    @pl.when(even)
    def _():
        seg_a().start()

    @pl.when(has_next)
    def _():
        seg_b().start()

    @pl.when(asks)
    def _():
        seg_d().start()

        def send_ask(j, carry):
            ask(turn(j, arriving)).start()
            return carry

        lax.fori_loop(0, turns, send_ask, 0)

    @pl.when(ships)
    def _():
        seg_e().start()
        ask_beside().start()

    @pl.when(ships & has_prev)
    def _():
        seg_d().start()
        ask(last).start()

    for i in range(deepest):
        for p in reversed(range(PIECES)):

            @pl.when(unit(i, p) < leaving)
            def _():
                flow_d(i, p).start()

    def send(h, carry):
        for p in range(PIECES):

            @pl.when(has_next & ((odd & ((h < last) | keeps)) | (h < KEPT)))
            def _():
                flow_b(h, p).start()

            @pl.when(even & ((h < last) | keeps))
            def _():
                flow_a(h, p).start()

        return carry

    lax.fori_loop(0, heads, send, 0)

    def arrive(h, pieces):
        for p in pieces:

            @pl.when(s >= 1)
            def _():
                flow_a(h, p).wait_recv()

    def reach(h, p):
        @pl.when(has_prev)
        def _():
            flow_b(h, p).wait_recv()

        @pl.when(forwards(h, p))
        def _():
            flow_c(h, p).start()

    def pass_on(h):
        for p in range(PIECES):
            reach(h, p)

    @pl.when(odd & has_prev)
    def _():
        seg_b().wait_recv()
        seg_c().start()
        pass_on(0)

    @pl.when(s < 1)
    def _():
        buf1[...] = jnp.zeros_like(buf1)
        seg1[...] = jnp.full_like(seg1, -1)

    @pl.when(s < 2)
    def _():
        buf2[...] = jnp.zeros_like(buf2)
        seg2[...] = jnp.full_like(seg2, -1)

    @pl.when(s == 0)
    def _():
        part_in[...] = jnp.zeros_like(part_in)
        lse_in[...] = jnp.full_like(lse_in, NEVER)

    @pl.when(s == 1)
    def _():
        part_in[last] = jnp.zeros((rows, HEAD_DIM), part_in.dtype)
        lse_in[last] = jnp.full((8, rows), NEVER, jnp.float32)

    def column(row):
        return jnp.transpose(jnp.broadcast_to(row, (HEAD_DIM, rows)))

    query_seg = column(seg_ref[...])[:, :1]
    query_pos = lax.broadcasted_iota(jnp.int32, (rows, rows), 0)
    key_pos = lax.broadcasted_iota(jnp.int32, (rows, rows), 1)
    allowed = (query_seg == seg_ref[...]) & (key_pos <= query_pos)
    bias[:, :rows] = jnp.where(allowed, 0.0, -jnp.inf)
    squares[...] = jnp.zeros_like(squares)
    image_ref[...] = column(mod_ref[...])

    def scores_of(query, key):
        return scale * lax.dot_general(
            query, key, (((1,), (1,)), ((), ())), preferred_element_type=jnp.float32
        )

    def relay_head(i):
        for p in reversed(range(PIECES)):

            @pl.when(unit(i, p) < passing)
            def _():
                flow_d(i, p).wait_recv()
                flow_e(i, p).start()

    def attend_for(i, h):
        key = own[h, :half].reshape(rows, HEAD_DIM)
        value = own[h, half:].reshape(rows, HEAD_DIM)
        score = scores_of(q_next[i], key) + bias_next[...]
        top = jnp.max(score, axis=1, keepdims=True)
        weight = jnp.exp(score - top)
        total = jnp.sum(weight, axis=1, keepdims=True)
        acc = jnp.dot(weight.astype(jnp.bfloat16), value, preferred_element_type=jnp.float32)
        part_out[i] = (acc * (1.0 / total)).astype(jnp.bfloat16)
        lse = jnp.broadcast_to(top + jnp.log(total), (rows, HEAD_DIM))
        lse_out[i] = jnp.transpose(lse)[:8]

    def mask_for(ids):
        asker = column(ids[...])[:, :1]
        bias_next[...] = jnp.where(asker == seg_ref[...], 0.0, NEVER)

    def send_answer(i):
        answer_lse(i).start()
        answer(i).start()

    @pl.when(serves)
    def _():
        seg_e().wait_recv()
        mask_for(seg_beside)
        ask_beside().wait_recv()
        attend_for(0, last)

    @pl.when(has_next & (even | ships))
    def _():
        seg_d().wait_recv()
        mask_for(seg_next)

    @pl.when(serves)
    def _():
        answer_beside_lse().start()
        answer_beside().start()

    @pl.when(ships & has_next)
    def _():
        ask(last).wait_recv()
        attend_for(last, last)

    @pl.when(answers)
    def _():
        def attend_next(j, carry):
            h = turn(j, passing)
            ask(h).wait_recv()
            attend_for(h, h)

            @pl.when(j > 0)
            def _():
                send_answer(turn(j - 1, passing))

            @pl.when((lax.rem(j, 2) == 0) & (j // 2 * PIECES < passing))
            def _():
                relay_head(j // 2)

            return carry

        lax.fori_loop(0, turns, attend_next, 0)
        send_answer(turn(turns - 1, passing))

    @pl.when(asks)
    def _():
        seg_b().wait_recv()

    @pl.when(s >= 1)
    def _():
        seg_a().wait_recv()

    bias[:, rows : 2 * rows] = jnp.where(query_seg == seg1[...], 0.0, -jnp.inf)
    bias[:, 2 * rows :] = jnp.where(query_seg == seg2[...], 0.0, -jnp.inf)

    def scores_with(h, block, i):
        key = block[h, :half].reshape(rows, HEAD_DIM)
        return scores_of(q_own[h], key) + bias[:, i * rows : (i + 1) * rows]

    def product(weight, value):
        return jnp.dot(weight.astype(jnp.bfloat16), value, preferred_element_type=jnp.float32)

    def values_of(block, h):
        return block[h, half:].reshape(rows, HEAD_DIM)

    def finish(h, acc, total):
        attended = (acc * (1.0 / total)).astype(jnp.bfloat16)
        att[h] = attended
        wide = attended.astype(jnp.float32)
        return wide * wide

    @pl.when(ships & has_next)
    def _():
        send_answer(last)

    def head(h):
        near = scores_with(h, own, 0)
        far = scores_with(h, buf2, 2)
        arrive(h, range(half))
        middle = scores_with(h, buf1, 1)
        top = jnp.max(jnp.maximum(jnp.maximum(near, middle), far), axis=1, keepdims=True)
        near = jnp.exp(near - top)
        far = jnp.exp(far - top)
        middle = jnp.exp(middle - top)
        total = jnp.sum(near + middle + far, axis=1, keepdims=True)
        acc = product(near, values_of(own, h))

        arrive(h, range(half, PIECES))
        acc = acc + product(far, values_of(buf2, h)) + product(middle, values_of(buf1, h))
        return finish(h, acc, total)

    def joined_last():
        near = scores_with(last, own, 0)
        top = jnp.max(near, axis=1, keepdims=True)
        near = jnp.exp(near - top)
        total = jnp.sum(near, axis=1, keepdims=True)
        acc = product(near, values_of(own, last))

        @pl.when(has_prev)
        def _():
            answer_lse(last).wait_recv()
            answer(last).wait_recv()

        answer_beside_lse().wait_recv()
        answer_beside().wait_recv()
        far_top = column(lse_in[last, :1])[:, :1]
        middle_top = column(lse_in[0, :1])[:, :1]
        most = jnp.maximum(top, jnp.maximum(far_top, middle_top))
        again = jnp.exp(top - most)
        far = jnp.exp(far_top - most)
        middle = jnp.exp(middle_top - most)
        total = again * total + far + middle
        acc = again * acc + far * part_in[last].astype(jnp.float32)
        acc = acc + middle * part_in[0].astype(jnp.float32)
        return finish(last, acc, total)

    def merged(h, apart):
        near = scores_with(h, own, 0)

        @pl.when(asks)
        def _():
            answer_lse(h).wait_recv()
            answer(h).wait_recv()

        lse = column(lse_in[h, :1])[:, :1]
        if not apart:
            arrive(h, range(half))
            middle = scores_with(h, buf1, 1)
            top = jnp.max(jnp.maximum(near, middle), axis=1, keepdims=True)
            top = jnp.maximum(top, lse)
            near = jnp.exp(near - top)
            middle = jnp.exp(middle - top)
            far = jnp.exp(lse - top)
            total = jnp.sum(near + middle, axis=1, keepdims=True) + far
            acc = product(near, values_of(own, h)) + far * part_in[h].astype(jnp.float32)
            arrive(h, range(half, PIECES))
            return finish(h, acc + product(middle, values_of(buf1, h)), total)
        first_top = jnp.maximum(jnp.max(near, axis=1, keepdims=True), lse)
        near = jnp.exp(near - first_top)
        far = jnp.exp(lse - first_top)
        first_total = jnp.sum(near, axis=1, keepdims=True) + far
        acc = product(near, values_of(own, h)) + far * part_in[h].astype(jnp.float32)
        arrive(h, range(half))
        middle = scores_with(h, buf1, 1)
        top = jnp.maximum(jnp.max(middle, axis=1, keepdims=True), first_top)
        middle = jnp.exp(middle - top)
        again = jnp.exp(first_top - top)
        total = jnp.sum(middle, axis=1, keepdims=True) + again * first_total
        acc = acc * again
        arrive(h, range(half, PIECES))
        return finish(h, acc + product(middle, values_of(buf1, h)), total)

    def one(h, carry):
        @pl.when(h + 1 < beside)
        def _():
            pass_on(h + 1)

        @pl.when(h >= beside)
        def _():
            pass_on(h)

        squares[...] += head(h)
        return carry

    def conclude(wide):
        partial = jnp.sum(squares[...] + wide, axis=1, keepdims=True)
        mine[...] = jnp.broadcast_to(partial, mine.shape)

    @pl.when(odd)
    def _():
        lax.fori_loop(0, last, one, 0)

        @pl.when(ships)
        def _():
            conclude(joined_last())

        @pl.when(keeps)
        def _():
            pass_on(last)
            conclude(head(last))

    def joined(j, carry):
        squares[...] += merged(turn(j, arriving), False)
        return carry

    @pl.when(even)
    def _():
        def kept(h, carry):
            pass_on(h)
            squares[...] += head(h)
            return carry

        lax.fori_loop(0, KEPT, kept, 0)
        lax.fori_loop(0, turns - 1, joined, 0)
        conclude(merged(turn(turns - 1, arriving), True))

    swap = pltpu.make_async_remote_copy(
        src_ref=mine,
        dst_ref=theirs,
        send_sem=sq_sem.at[0],
        recv_sem=sq_sem.at[1],
        device_id={"tp": 1 - t},
        device_id_type=MESH,
    )
    swap.start()

    def sent(ref, send):
        remote(ref, ref, send, recv_1.at[0, 0], pair).wait_send()

    for i in range(deepest):
        for p in range(PIECES):

            @pl.when(unit(i, p) < leaving)
            def _():
                flow_d(i, p).wait_send()

            @pl.when(unit(i, p) < passing)
            def _():
                flow_e(i, p).wait_send()

    @pl.when(asks)
    def _():
        seg_d().wait_send()
        for i in range(KEPT, heads):
            ask(i).wait_send()

    @pl.when(ships)
    def _():
        seg_e().wait_send()
        ask_beside().wait_send()

    @pl.when(ships & has_prev)
    def _():
        seg_d().wait_send()
        ask(last).wait_send()

    @pl.when(ships & has_next)
    def _():
        answer(last).wait_send()
        answer_lse(last).wait_send()

    @pl.when(answers)
    def _():
        for i in range(KEPT, heads):
            answer(i).wait_send()
            answer_lse(i).wait_send()

    @pl.when(even)
    def _():
        seg_a().wait_send()
        sent(own.at[:last], send_a)

    @pl.when(even & keeps)
    def _():
        sent(own.at[last], send_a)

    @pl.when(serves)
    def _():
        answer_beside().wait_send()
        answer_beside_lse().wait_send()

    @pl.when(has_next)
    def _():
        seg_b().wait_send()
        sent(own.at[:KEPT], send_b)

    @pl.when(odd & has_next)
    def _():
        sent(own.at[KEPT:last], send_b)

    @pl.when(odd & has_next & keeps)
    def _():
        sent(own.at[last], send_b)

    @pl.when(odd & has_prev)
    def _():
        seg_c().wait_send()

    for h in range(heads):
        for p in range(PIECES):

            @pl.when(forwards(h, p))
            def _():
                flow_c(h, p).wait_send()

    swap.wait_recv()
    mean_square = (mine[...] + theirs[...]) / (HEADS * HEAD_DIM)
    inverse_ref[...] = lax.rsqrt(mean_square + 1e-05)
    swap.wait_send()


def blend(heads, att, inverse_ref, image_ref, gain_ref, out_hbm, staged, out_sem):
    inverse = inverse_ref[...]
    image = image_ref[...] == 1
    copies = []
    for h in range(heads):
        columns = slice(h * HEAD_DIM, (h + 1) * HEAD_DIM)
        gain = jnp.where(image, gain_ref[1:2, columns], gain_ref[0:1, columns])
        staged[h] = (att[h].astype(jnp.float32) * inverse * gain).astype(staged.dtype)
        copy = pltpu.make_async_copy(
            staged.at[h], out_hbm.at[:, pl.ds(h * HEAD_DIM, HEAD_DIM)], out_sem.at[h]
        )
        copy.start()
        copies.append(copy)
    for copy in copies:
        copy.wait()


def on_device(n, queries, keys, values, segment_ids, modality, norm_gain):
    rows, width = queries.shape
    heads = width // HEAD_DIM
    vmem = pl.BlockSpec(memory_space=pltpu.VMEM)
    hbm = pl.BlockSpec(memory_space=pltpu.HBM)
    depth = 2 * rows // PIECES
    block = pltpu.VMEM((heads, PIECES, depth, HEAD_DIM), jnp.bfloat16)
    deepest = (max(MOST + LEAST) + PIECES - 1) // PIECES
    asked = pltpu.VMEM((heads, rows, HEAD_DIM), jnp.bfloat16)
    ids = pltpu.VMEM((1, rows), jnp.int32)
    flow = pltpu.SemaphoreType.DMA((heads, PIECES))
    att, inverse, image = pl.pallas_call(
        functools.partial(kernel, n, heads, rows),
        out_shape=(
            pltpu.VMEM((heads, rows, HEAD_DIM), jnp.bfloat16),
            pltpu.VMEM((rows, HEAD_DIM), jnp.float32),
            pltpu.VMEM((rows, HEAD_DIM), jnp.int32),
        ),
        in_specs=[hbm, hbm, hbm, hbm, hbm],
        out_specs=(vmem, vmem, vmem),
        scratch_shapes=[
            pltpu.VMEM((heads, rows, HEAD_DIM), jnp.bfloat16),
            block,
            block,
            block,
            pltpu.VMEM((deepest, PIECES, depth, HEAD_DIM), jnp.bfloat16),
            asked,
            asked,
            pltpu.VMEM((heads, 8, rows), jnp.float32),
            asked,
            pltpu.VMEM((heads, 8, rows), jnp.float32),
            ids,
            ids,
            ids,
            ids,
            ids,
            ids,
            pltpu.VMEM((rows, (REACH + 1) * rows), jnp.float32),
            pltpu.VMEM((rows, rows), jnp.float32),
            pltpu.VMEM((rows, HEAD_DIM), jnp.float32),
            pltpu.VMEM((rows, HEAD_DIM), jnp.float32),
            pltpu.VMEM((rows, HEAD_DIM), jnp.float32),
            pltpu.SemaphoreType.DMA,
            pltpu.SemaphoreType.DMA,
            pltpu.SemaphoreType.DMA,
            pltpu.SemaphoreType.DMA,
            flow,
            flow,
            flow,
            pltpu.SemaphoreType.DMA((deepest, PIECES)),
            pltpu.SemaphoreType.DMA((deepest, PIECES)),
            pltpu.SemaphoreType.DMA((2, heads)),
            pltpu.SemaphoreType.DMA((2, heads)),
            pltpu.SemaphoreType.DMA((2, heads)),
            pltpu.SemaphoreType.DMA((2,)),
            pltpu.SemaphoreType.DMA((5,)),
            pltpu.SemaphoreType.DMA((4,)),
            pltpu.SemaphoreType.DMA((2,)),
        ],
        compiler_params=pltpu.CompilerParams(
            collective_id=0, has_side_effects=True
        ),
    )(queries, keys, values, segment_ids.reshape(1, rows), modality.reshape(1, rows))
    return pl.pallas_call(
        functools.partial(blend, heads),
        out_shape=jax.ShapeDtypeStruct((rows, width), jnp.bfloat16),
        in_specs=[vmem, vmem, vmem, vmem],
        out_specs=hbm,
        scratch_shapes=[
            pltpu.VMEM((heads, rows, HEAD_DIM), jnp.bfloat16),
            pltpu.SemaphoreType.DMA((heads,)),
        ],
        compiler_params=pltpu.CompilerParams(vmem_limit_bytes=8 * 2**20),
    )(att, inverse, image, norm_gain)


def solution(mesh):
    return jax.shard_map(
        functools.partial(on_device, mesh.shape["seq"]),
        mesh=mesh,
        in_specs=(
            P(("grp", "seq"), "tp"),
            P(("grp", "seq"), "tp"),
            P(("grp", "seq"), "tp"),
            P(("grp", "seq")),
            P(("grp", "seq")),
            P(None, "tp"),
        ),
        out_specs=P(("grp", "seq"), "tp"),
        check_vma=False,
    )
```

```python
import functools

import jax
import jax.numpy as jnp
from jax import lax
from jax.experimental import pallas as pl
from jax.experimental.pallas import tpu as pltpu
from jax.sharding import PartitionSpec as P

HEADS = 16
HEAD_DIM = 128
REACH = 2
MESH = pl.DeviceIdType.MESH
PIECES = 2
MOST = (4, 6)
LEAST = (4, 2)
NEVER = -1e30
FOLD = 4
KEPT = 2
SHIPPER = 0


def kernel(
    n,
    heads,
    rows,
    q_hbm,
    k_hbm,
    v_hbm,
    seg_hbm,
    mod_hbm,
    att,
    inverse_ref,
    image_ref,
    q_own,
    own,
    buf1,
    buf2,
    hop,
    q_next,
    part_out,
    lse_out,
    part_in,
    lse_in,
    seg_ref,
    mod_ref,
    seg1,
    seg2,
    seg_next,
    seg_beside,
    bias,
    bias_next,
    squares,
    mine,
    theirs,
    own_sem,
    q_sem,
    send_a,
    send_b,
    send_c,
    recv_1,
    recv_2,
    hop_send,
    hop_recv,
    ask_sem,
    part_sem,
    lse_sem,
    id_sem,
    seg_send,
    seg_recv,
    sq_sem,
):
    s = lax.axis_index("seq")
    t = lax.axis_index("tp")
    even = lax.rem(s, 2) == 0
    odd = lax.rem(s, 2) == 1
    has_next = s + 2 < n
    has_prev = s >= 2
    ahead = odd & (s + 1 < n)
    behind = even & has_prev
    asks = even & has_prev
    answers = even & has_next
    pair = s + 1 - 2 * lax.rem(s, 2)
    ships = odd & (t == SHIPPER)
    serves = even & (t == SHIPPER)
    keeps = t != SHIPPER

    deep = rows // FOLD
    half = PIECES // 2
    depth = rows // half
    last = heads - 1
    turns = heads - KEPT
    cuts = n // 2 - 1
    scale = HEAD_DIM ** (-0.5)

    def direct_into(block):
        top = jnp.where(t == 0, MOST[0], MOST[1])
        low = jnp.where(t == 0, LEAST[0], LEAST[1])
        return low + ((cuts - block // 2) * (top - low)) // max(cuts - 1, 1)

    deepest = (max(MOST + LEAST) + PIECES - 1) // PIECES
    leaving = jnp.where(ahead, direct_into(s + 1), 0)
    passing = jnp.where(even & has_next, direct_into(s + 2), 0)
    arriving = jnp.where(asks, direct_into(s), 0)
    skipped = jnp.where(odd & has_prev, direct_into(s - 1), 0)
    beside = heads - skipped // PIECES

    def unit(i, p):
        return PIECES * i + PIECES - 1 - p

    def turn(j, direct):
        mixed = jnp.where(lax.rem(j, 2) == 0, last - j // 2, KEPT + j // 2)
        return jnp.where(j < 2 * (direct // PIECES), mixed, KEPT + j - direct // PIECES)

    def columns_of(h):
        return pl.ds(h * HEAD_DIM, HEAD_DIM)

    def load_piece(h, p):
        source = k_hbm if p < half else v_hbm
        piece = pl.ds((p % half) * depth, depth)
        return pltpu.make_async_copy(
            source.at[piece, columns_of(h)], own.at[h, p], own_sem
        )

    def load_q(h):
        return pltpu.make_async_copy(q_hbm.at[:, columns_of(h)], q_own.at[h], q_sem)

    def load_ids(i):
        source, target = ((seg_hbm, seg_ref), (mod_hbm, mod_ref))[i]
        return pltpu.make_async_copy(source, target, id_sem.at[i])

    barrier = pltpu.get_barrier_semaphore()
    peers = (
        (None, {"tp": 1 - t}),
        (None, {"seq": pair}),
        (has_next, {"seq": s + 2}),
        (has_prev, {"seq": s - 2}),
    )
    expected = 0
    for condition, peer in peers:

        def greet(peer=peer):
            pl.semaphore_signal(barrier, inc=1, device_id=peer, device_id_type=MESH)

        if condition is None:
            greet()
            expected = expected + 1
        else:
            pl.when(condition)(greet)
            expected = expected + jnp.where(condition, 1, 0)

    load_ids(0).start()
    for h in range(heads):
        for p in range(PIECES):
            load_piece(h, p).start()
        load_q(h).start()
    load_ids(1).start()
    for i in (0, 1):
        load_ids(i).wait()
    pltpu.make_async_copy(own, own, own_sem).wait()
    pltpu.make_async_copy(q_own, q_own, q_sem).wait()
    pl.semaphore_wait(barrier, expected)

    def remote(source, target, send, recv, where):
        return pltpu.make_async_remote_copy(
            src_ref=source,
            dst_ref=target,
            send_sem=send,
            recv_sem=recv,
            device_id={"seq": where},
            device_id_type=MESH,
        )

    def flow_a(h, p):
        return remote(own.at[h, p], buf1.at[h, p], send_a, recv_1.at[h, p], pair)

    def flow_b(h, p):
        return remote(own.at[h, p], buf2.at[h, p], send_b, recv_2.at[h, p], s + 2)

    def flow_c(h, p):
        return remote(buf2.at[h, p], buf1.at[h, p], send_c.at[h, p], recv_1.at[h, p], pair)

    def flow_d(i, p):
        return remote(
            own.at[last - i, p], hop.at[i, p], hop_send.at[i, p], hop_recv.at[i, p], pair
        )

    def flow_e(i, p):
        return remote(
            hop.at[i, p], buf1.at[last - i, p], hop_send.at[i, p], recv_1.at[last - i, p], s + 2
        )

    def ask(i):
        return remote(
            q_own.at[i], q_next.at[i], ask_sem.at[0, i], ask_sem.at[1, i], s - 2
        )

    def answer(i):
        return remote(
            part_out.at[i], part_in.at[i], part_sem.at[0, i], part_sem.at[1, i], s + 2
        )

    def ask_beside():
        return remote(q_own.at[last], q_next.at[0], ask_sem.at[0, 0], ask_sem.at[1, 0], pair)

    def answer_beside():
        return remote(part_out.at[0], part_in.at[0], part_sem.at[0, 0], part_sem.at[1, 0], pair)

    def answer_beside_lse():
        return remote(lse_out.at[0], lse_in.at[0], lse_sem.at[0, 0], lse_sem.at[1, 0], pair)

    def answer_lse(i):
        return remote(lse_out.at[i], lse_in.at[i], lse_sem.at[0, i], lse_sem.at[1, i], s + 2)

    def forwards(h, p):
        return odd & has_prev & (unit(last - h, p) >= skipped)

    def seg_a():
        return remote(seg_ref, seg1, seg_send.at[0], seg_recv.at[0], pair)

    def seg_b():
        return remote(seg_ref, seg2, seg_send.at[1], seg_recv.at[1], s + 2)

    def seg_c():
        return remote(seg2, seg1, seg_send.at[2], seg_recv.at[0], pair)

    def seg_e():
        return remote(seg_ref, seg_beside, seg_send.at[4], seg_recv.at[3], pair)

    def seg_d():
        return remote(seg_ref, seg_next, seg_send.at[3], seg_recv.at[2], s - 2)

    @pl.when(even)
    def _():
        seg_a().start()

    @pl.when(has_next)
    def _():
        seg_b().start()

    @pl.when(asks)
    def _():
        seg_d().start()

        def send_ask(j, carry):
            ask(turn(j, arriving)).start()
            return carry

        lax.fori_loop(0, turns, send_ask, 0)

    @pl.when(ships)
    def _():
        seg_e().start()
        ask_beside().start()

    @pl.when(ships & has_prev)
    def _():
        seg_d().start()
        ask(last).start()

    for i in range(deepest):
        for p in reversed(range(PIECES)):

            @pl.when(unit(i, p) < leaving)
            def _():
                flow_d(i, p).start()

    def send(h, carry):
        for p in range(PIECES):

            @pl.when(has_next & ((odd & ((h < last) | keeps)) | (h < KEPT)))
            def _():
                flow_b(h, p).start()

            @pl.when(even & ((h < last) | keeps))
            def _():
                flow_a(h, p).start()

        return carry

    lax.fori_loop(0, heads, send, 0)

    def arrive(h, pieces):
        for p in pieces:

            @pl.when(s >= 1)
            def _():
                flow_a(h, p).wait_recv()

    def reach(h, p):
        @pl.when(has_prev)
        def _():
            flow_b(h, p).wait_recv()

        @pl.when(forwards(h, p))
        def _():
            flow_c(h, p).start()

    def pass_on(h):
        for p in range(PIECES):
            reach(h, p)

    @pl.when(odd & has_prev)
    def _():
        seg_b().wait_recv()
        seg_c().start()
        pass_on(0)

    @pl.when(s < 1)
    def _():
        buf1[...] = jnp.zeros_like(buf1)
        seg1[...] = jnp.full_like(seg1, -1)

    @pl.when(s < 2)
    def _():
        buf2[...] = jnp.zeros_like(buf2)
        seg2[...] = jnp.full_like(seg2, -1)

    @pl.when(s == 0)
    def _():
        part_in[...] = jnp.zeros_like(part_in)
        lse_in[...] = jnp.full_like(lse_in, NEVER)

    @pl.when(s == 1)
    def _():
        part_in[last] = jnp.zeros((rows, HEAD_DIM), part_in.dtype)
        lse_in[last] = jnp.full((8, rows), NEVER, jnp.float32)

    def column(row):
        return jnp.transpose(jnp.broadcast_to(row, (HEAD_DIM, rows)))

    query_seg = column(seg_ref[...])[:, :1]
    query_pos = lax.broadcasted_iota(jnp.int32, (rows, rows), 0)
    key_pos = lax.broadcasted_iota(jnp.int32, (rows, rows), 1)
    allowed = (query_seg == seg_ref[...]) & (key_pos <= query_pos)
    bias[:, :rows] = jnp.where(allowed, 0.0, -jnp.inf)
    squares[...] = jnp.zeros_like(squares)
    image_ref[...] = column(mod_ref[...])

    def scores_of(query, key):
        return scale * lax.dot_general(
            query, key, (((1,), (1,)), ((), ())), preferred_element_type=jnp.float32
        )

    def relay_head(i):
        for p in reversed(range(PIECES)):

            @pl.when(unit(i, p) < passing)
            def _():
                flow_d(i, p).wait_recv()
                flow_e(i, p).start()

    def attend_for(i, h):
        key = own[h, :half].reshape(rows, HEAD_DIM)
        value = own[h, half:].reshape(rows, HEAD_DIM)
        score = scores_of(q_next[i], key) + bias_next[...]
        top = jnp.max(score, axis=1, keepdims=True)
        weight = jnp.exp(score - top)
        total = jnp.sum(weight, axis=1, keepdims=True)
        acc = jnp.dot(weight.astype(jnp.bfloat16), value, preferred_element_type=jnp.float32)
        part_out[i] = (acc * (1.0 / total)).astype(jnp.bfloat16)
        lse = jnp.broadcast_to(top + jnp.log(total), (rows, HEAD_DIM))
        lse_out[i] = jnp.transpose(lse)[:8]

    def mask_for(ids):
        asker = column(ids[...])[:, :1]
        bias_next[...] = jnp.where(asker == seg_ref[...], 0.0, NEVER)

    def send_answer(i):
        answer_lse(i).start()
        answer(i).start()

    @pl.when(serves)
    def _():
        seg_e().wait_recv()
        mask_for(seg_beside)
        ask_beside().wait_recv()
        attend_for(0, last)

    @pl.when(has_next & (even | ships))
    def _():
        seg_d().wait_recv()
        mask_for(seg_next)

    @pl.when(ships & has_next)
    def _():
        ask(last).wait_recv()
        attend_for(last, last)

    @pl.when(answers)
    def _():
        def attend_next(j, carry):
            h = turn(j, passing)
            ask(h).wait_recv()
            attend_for(h, h)

            @pl.when(j > 0)
            def _():
                send_answer(turn(j - 1, passing))

            @pl.when((lax.rem(j, 2) == 0) & (j // 2 * PIECES < passing))
            def _():
                relay_head(j // 2)

            return carry

        lax.fori_loop(0, turns, attend_next, 0)
        send_answer(turn(turns - 1, passing))

    @pl.when(asks)
    def _():
        seg_b().wait_recv()

    @pl.when(s >= 1)
    def _():
        seg_a().wait_recv()

    bias[:, rows : 2 * rows] = jnp.where(query_seg == seg1[...], 0.0, -jnp.inf)
    bias[:, 2 * rows :] = jnp.where(query_seg == seg2[...], 0.0, -jnp.inf)

    def scores_with(h, block, i):
        key = block[h, :half].reshape(rows, HEAD_DIM)
        return scores_of(q_own[h], key) + bias[:, i * rows : (i + 1) * rows]

    def product(weight, value):
        return jnp.dot(weight.astype(jnp.bfloat16), value, preferred_element_type=jnp.float32)

    def values_of(block, h):
        return block[h, half:].reshape(rows, HEAD_DIM)

    def finish(h, acc, total):
        attended = (acc * (1.0 / total)).astype(jnp.bfloat16)
        att[h] = attended
        wide = attended.astype(jnp.float32)
        return wide * wide

    @pl.when(ships & has_next)
    def _():
        send_answer(last)

    @pl.when(serves)
    def _():
        answer_beside_lse().start()
        answer_beside().start()

    def head(h):
        near = scores_with(h, own, 0)
        far = scores_with(h, buf2, 2)
        arrive(h, range(half))
        middle = scores_with(h, buf1, 1)
        top = jnp.max(jnp.maximum(jnp.maximum(near, middle), far), axis=1, keepdims=True)
        near = jnp.exp(near - top)
        far = jnp.exp(far - top)
        middle = jnp.exp(middle - top)
        total = jnp.sum(near + middle + far, axis=1, keepdims=True)
        acc = product(near, values_of(own, h))

        arrive(h, range(half, PIECES))
        acc = acc + product(far, values_of(buf2, h)) + product(middle, values_of(buf1, h))
        return finish(h, acc, total)

    def joined_last():
        near = scores_with(last, own, 0)
        top = jnp.max(near, axis=1, keepdims=True)
        near = jnp.exp(near - top)
        total = jnp.sum(near, axis=1, keepdims=True)
        acc = product(near, values_of(own, last))

        @pl.when(has_prev)
        def _():
            answer_lse(last).wait_recv()
            answer(last).wait_recv()

        answer_beside_lse().wait_recv()
        answer_beside().wait_recv()
        far_top = column(lse_in[last, :1])[:, :1]
        middle_top = column(lse_in[0, :1])[:, :1]
        most = jnp.maximum(top, jnp.maximum(far_top, middle_top))
        again = jnp.exp(top - most)
        far = jnp.exp(far_top - most)
        middle = jnp.exp(middle_top - most)
        total = again * total + far + middle
        acc = again * acc + far * part_in[last].astype(jnp.float32)
        acc = acc + middle * part_in[0].astype(jnp.float32)
        return finish(last, acc, total)

    def merged(h, apart):
        near = scores_with(h, own, 0)

        @pl.when(asks)
        def _():
            answer_lse(h).wait_recv()
            answer(h).wait_recv()

        lse = column(lse_in[h, :1])[:, :1]
        if not apart:
            arrive(h, range(half))
            middle = scores_with(h, buf1, 1)
            top = jnp.max(jnp.maximum(near, middle), axis=1, keepdims=True)
            top = jnp.maximum(top, lse)
            near = jnp.exp(near - top)
            middle = jnp.exp(middle - top)
            far = jnp.exp(lse - top)
            total = jnp.sum(near + middle, axis=1, keepdims=True) + far
            acc = product(near, values_of(own, h)) + far * part_in[h].astype(jnp.float32)
            arrive(h, range(half, PIECES))
            return finish(h, acc + product(middle, values_of(buf1, h)), total)
        first_top = jnp.maximum(jnp.max(near, axis=1, keepdims=True), lse)
        near = jnp.exp(near - first_top)
        far = jnp.exp(lse - first_top)
        first_total = jnp.sum(near, axis=1, keepdims=True) + far
        acc = product(near, values_of(own, h)) + far * part_in[h].astype(jnp.float32)
        arrive(h, range(half))
        middle = scores_with(h, buf1, 1)
        top = jnp.maximum(jnp.max(middle, axis=1, keepdims=True), first_top)
        middle = jnp.exp(middle - top)
        again = jnp.exp(first_top - top)
        total = jnp.sum(middle, axis=1, keepdims=True) + again * first_total
        acc = acc * again
        arrive(h, range(half, PIECES))
        return finish(h, acc + product(middle, values_of(buf1, h)), total)

    def one(h, carry):
        @pl.when(h + 1 < beside)
        def _():
            pass_on(h + 1)

        @pl.when(h >= beside)
        def _():
            pass_on(h)

        squares[...] += head(h)
        return carry

    def conclude(wide):
        partial = jnp.sum(squares[...] + wide, axis=1, keepdims=True)
        strip = lax.broadcasted_iota(jnp.int32, mine.shape, 1) // (HEAD_DIM // FOLD)
        folded = jnp.broadcast_to(partial[:deep], mine.shape)
        for g in range(1, FOLD):
            folded = jnp.where(strip == g, partial[g * deep : (g + 1) * deep], folded)
        mine[...] = folded

    @pl.when(odd)
    def _():
        lax.fori_loop(0, last, one, 0)

        @pl.when(ships)
        def _():
            conclude(joined_last())

        @pl.when(keeps)
        def _():
            @pl.when(beside < heads)
            def _():
                pass_on(last)

            conclude(head(last))

    def joined(j, carry):
        squares[...] += merged(turn(j, arriving), False)
        return carry

    @pl.when(even)
    def _():
        def kept(h, carry):
            pass_on(h)
            squares[...] += head(h)
            return carry

        lax.fori_loop(0, KEPT, kept, 0)
        lax.fori_loop(0, turns - 1, joined, 0)
        conclude(merged(turn(turns - 1, arriving), True))

    swap = pltpu.make_async_remote_copy(
        src_ref=mine,
        dst_ref=theirs,
        send_sem=sq_sem.at[0],
        recv_sem=sq_sem.at[1],
        device_id={"tp": 1 - t},
        device_id_type=MESH,
    )
    swap.start()

    def sent(ref, send):
        remote(ref, ref, send, recv_1.at[0, 0], pair).wait_send()

    for i in range(deepest):
        for p in range(PIECES):

            @pl.when(unit(i, p) < leaving)
            def _():
                flow_d(i, p).wait_send()

            @pl.when(unit(i, p) < passing)
            def _():
                flow_e(i, p).wait_send()

    @pl.when(asks)
    def _():
        seg_d().wait_send()
        for i in range(KEPT, heads):
            ask(i).wait_send()

    @pl.when(ships)
    def _():
        seg_e().wait_send()
        ask_beside().wait_send()

    @pl.when(ships & has_prev)
    def _():
        seg_d().wait_send()
        ask(last).wait_send()

    @pl.when(ships & has_next)
    def _():
        answer(last).wait_send()
        answer_lse(last).wait_send()

    @pl.when(answers)
    def _():
        for i in range(KEPT, heads):
            answer(i).wait_send()
            answer_lse(i).wait_send()

    @pl.when(even)
    def _():
        seg_a().wait_send()
        sent(own.at[:last], send_a)

    @pl.when(even & keeps)
    def _():
        sent(own.at[last], send_a)

    @pl.when(serves)
    def _():
        answer_beside().wait_send()
        answer_beside_lse().wait_send()

    @pl.when(has_next)
    def _():
        seg_b().wait_send()
        sent(own.at[:KEPT], send_b)

    @pl.when(odd & has_next)
    def _():
        sent(own.at[KEPT:last], send_b)

    @pl.when(odd & has_next & keeps)
    def _():
        sent(own.at[last], send_b)

    @pl.when(odd & has_prev)
    def _():
        seg_c().wait_send()

    for h in range(heads):
        for p in range(PIECES):

            @pl.when(forwards(h, p))
            def _():
                flow_c(h, p).wait_send()

    swap.wait_recv()
    mean_square = (mine[...] + theirs[...]) / (HEADS * HEAD_DIM)
    inverse = lax.rsqrt(mean_square + 1e-05)
    for g in range(FOLD):
        lane = g * (HEAD_DIM // FOLD)
        inverse_ref[g * deep : (g + 1) * deep] = jnp.broadcast_to(
            inverse[:, lane : lane + 1], (deep, HEAD_DIM)
        )
    swap.wait_send()


def blend(heads, att, inverse_ref, image_ref, gain_ref, out_hbm, staged, out_sem):
    inverse = inverse_ref[...]
    image = image_ref[...] == 1
    copies = []
    for h in range(heads):
        columns = slice(h * HEAD_DIM, (h + 1) * HEAD_DIM)
        gain = jnp.where(image, gain_ref[1:2, columns], gain_ref[0:1, columns])
        staged[h] = (att[h].astype(jnp.float32) * inverse * gain).astype(staged.dtype)
        copy = pltpu.make_async_copy(
            staged.at[h], out_hbm.at[:, pl.ds(h * HEAD_DIM, HEAD_DIM)], out_sem.at[h]
        )
        copy.start()
        copies.append(copy)
    for copy in copies:
        copy.wait()


def on_device(n, queries, keys, values, segment_ids, modality, norm_gain):
    rows, width = queries.shape
    heads = width // HEAD_DIM
    vmem = pl.BlockSpec(memory_space=pltpu.VMEM)
    hbm = pl.BlockSpec(memory_space=pltpu.HBM)
    depth = 2 * rows // PIECES
    block = pltpu.VMEM((heads, PIECES, depth, HEAD_DIM), jnp.bfloat16)
    deepest = (max(MOST + LEAST) + PIECES - 1) // PIECES
    asked = pltpu.VMEM((heads, rows, HEAD_DIM), jnp.bfloat16)
    ids = pltpu.VMEM((1, rows), jnp.int32)
    flow = pltpu.SemaphoreType.DMA((heads, PIECES))
    att, inverse, image = pl.pallas_call(
        functools.partial(kernel, n, heads, rows),
        out_shape=(
            pltpu.VMEM((heads, rows, HEAD_DIM), jnp.bfloat16),
            pltpu.VMEM((rows, HEAD_DIM), jnp.float32),
            pltpu.VMEM((rows, HEAD_DIM), jnp.int32),
        ),
        in_specs=[hbm, hbm, hbm, hbm, hbm],
        out_specs=(vmem, vmem, vmem),
        scratch_shapes=[
            pltpu.VMEM((heads, rows, HEAD_DIM), jnp.bfloat16),
            block,
            block,
            block,
            pltpu.VMEM((deepest, PIECES, depth, HEAD_DIM), jnp.bfloat16),
            asked,
            asked,
            pltpu.VMEM((heads, 8, rows), jnp.float32),
            asked,
            pltpu.VMEM((heads, 8, rows), jnp.float32),
            ids,
            ids,
            ids,
            ids,
            ids,
            ids,
            pltpu.VMEM((rows, (REACH + 1) * rows), jnp.float32),
            pltpu.VMEM((rows, rows), jnp.float32),
            pltpu.VMEM((rows, HEAD_DIM), jnp.float32),
            pltpu.VMEM((rows // FOLD, HEAD_DIM), jnp.float32),
            pltpu.VMEM((rows // FOLD, HEAD_DIM), jnp.float32),
            pltpu.SemaphoreType.DMA,
            pltpu.SemaphoreType.DMA,
            pltpu.SemaphoreType.DMA,
            pltpu.SemaphoreType.DMA,
            flow,
            flow,
            flow,
            pltpu.SemaphoreType.DMA((deepest, PIECES)),
            pltpu.SemaphoreType.DMA((deepest, PIECES)),
            pltpu.SemaphoreType.DMA((2, heads)),
            pltpu.SemaphoreType.DMA((2, heads)),
            pltpu.SemaphoreType.DMA((2, heads)),
            pltpu.SemaphoreType.DMA((2,)),
            pltpu.SemaphoreType.DMA((5,)),
            pltpu.SemaphoreType.DMA((4,)),
            pltpu.SemaphoreType.DMA((2,)),
        ],
        compiler_params=pltpu.CompilerParams(
            collective_id=0, has_side_effects=True
        ),
    )(queries, keys, values, segment_ids.reshape(1, rows), modality.reshape(1, rows))
    return pl.pallas_call(
        functools.partial(blend, heads),
        out_shape=jax.ShapeDtypeStruct((rows, width), jnp.bfloat16),
        in_specs=[vmem, vmem, vmem, vmem],
        out_specs=hbm,
        scratch_shapes=[
            pltpu.VMEM((heads, rows, HEAD_DIM), jnp.bfloat16),
            pltpu.SemaphoreType.DMA((heads,)),
        ],
        compiler_params=pltpu.CompilerParams(vmem_limit_bytes=8 * 2**20),
    )(att, inverse, image, norm_gain)


def solution(mesh):
    return jax.shard_map(
        functools.partial(on_device, mesh.shape["seq"]),
        mesh=mesh,
        in_specs=(
            P(("grp", "seq"), "tp"),
            P(("grp", "seq"), "tp"),
            P(("grp", "seq"), "tp"),
            P(("grp", "seq")),
            P(("grp", "seq")),
            P(None, "tp"),
        ),
        out_specs=P(("grp", "seq"), "tp"),
        check_vma=False,
    )
```

```python
import functools

import jax
import jax.numpy as jnp
from jax import lax
from jax.experimental import pallas as pl
from jax.experimental.pallas import tpu as pltpu
from jax.sharding import PartitionSpec as P

HEADS = 16
HEAD_DIM = 128
REACH = 2
MESH = pl.DeviceIdType.MESH
PIECES = 2
MOST = (4, 6)
LEAST = (4, 2)
NEVER = -1e30
FOLD = 4
KEPT = 2
SHIPPER = 0


def kernel(
    n,
    heads,
    rows,
    q_hbm,
    k_hbm,
    v_hbm,
    seg_hbm,
    mod_hbm,
    att,
    inverse_ref,
    image_ref,
    q_own,
    own,
    buf1,
    buf2,
    hop,
    q_next,
    part_out,
    lse_out,
    part_in,
    lse_in,
    seg_ref,
    mod_ref,
    seg1,
    seg2,
    seg_next,
    seg_beside,
    bias,
    bias_next,
    squares,
    mine,
    theirs,
    own_sem,
    q_sem,
    send_a,
    send_b,
    send_c,
    recv_1,
    recv_2,
    hop_send,
    hop_recv,
    ask_sem,
    part_sem,
    lse_sem,
    id_sem,
    seg_send,
    seg_recv,
    sq_sem,
):
    s = lax.axis_index("seq")
    t = lax.axis_index("tp")
    even = lax.rem(s, 2) == 0
    odd = lax.rem(s, 2) == 1
    has_next = s + 2 < n
    has_prev = s >= 2
    ahead = odd & (s + 1 < n)
    behind = even & has_prev
    asks = even & has_prev
    answers = even & has_next
    pair = s + 1 - 2 * lax.rem(s, 2)
    ships = odd & (t == SHIPPER)
    serves = even & (t == SHIPPER)
    keeps = t != SHIPPER

    deep = rows // FOLD
    half = PIECES // 2
    depth = rows // half
    last = heads - 1
    turns = heads - KEPT
    cuts = n // 2 - 1
    scale = HEAD_DIM ** (-0.5)

    def direct_into(block):
        top = jnp.where(t == 0, MOST[0], MOST[1])
        low = jnp.where(t == 0, LEAST[0], LEAST[1])
        return low + ((cuts - block // 2) * (top - low)) // max(cuts - 1, 1)

    deepest = (max(MOST + LEAST) + PIECES - 1) // PIECES
    leaving = jnp.where(ahead, direct_into(s + 1), 0)
    passing = jnp.where(even & has_next, direct_into(s + 2), 0)
    arriving = jnp.where(asks, direct_into(s), 0)
    skipped = jnp.where(odd & has_prev, direct_into(s - 1), 0)
    beside = heads - skipped // PIECES

    def unit(i, p):
        return PIECES * i + PIECES - 1 - p

    def turn(j, direct):
        mixed = jnp.where(lax.rem(j, 2) == 0, last - j // 2, KEPT + j // 2)
        return jnp.where(j < 2 * (direct // PIECES), mixed, KEPT + j - direct // PIECES)

    def columns_of(h):
        return pl.ds(h * HEAD_DIM, HEAD_DIM)

    def load_piece(h, p):
        source = k_hbm if p < half else v_hbm
        piece = pl.ds((p % half) * depth, depth)
        return pltpu.make_async_copy(
            source.at[piece, columns_of(h)], own.at[h, p], own_sem
        )

    def load_q(h):
        return pltpu.make_async_copy(q_hbm.at[:, columns_of(h)], q_own.at[h], q_sem)

    def load_ids(i):
        source, target = ((seg_hbm, seg_ref), (mod_hbm, mod_ref))[i]
        return pltpu.make_async_copy(source, target, id_sem.at[i])

    barrier = pltpu.get_barrier_semaphore()
    peers = (
        (None, {"tp": 1 - t}),
        (None, {"seq": pair}),
        (has_next, {"seq": s + 2}),
        (has_prev, {"seq": s - 2}),
    )
    expected = 0
    for condition, peer in peers:

        def greet(peer=peer):
            pl.semaphore_signal(barrier, inc=1, device_id=peer, device_id_type=MESH)

        if condition is None:
            greet()
            expected = expected + 1
        else:
            pl.when(condition)(greet)
            expected = expected + jnp.where(condition, 1, 0)

    load_ids(0).start()
    for h in range(heads):
        for p in range(PIECES):
            load_piece(h, p).start()
        load_q(h).start()
    load_ids(1).start()
    for i in (0, 1):
        load_ids(i).wait()
    pltpu.make_async_copy(own, own, own_sem).wait()
    pltpu.make_async_copy(q_own, q_own, q_sem).wait()
    pl.semaphore_wait(barrier, expected)

    def remote(source, target, send, recv, where):
        return pltpu.make_async_remote_copy(
            src_ref=source,
            dst_ref=target,
            send_sem=send,
            recv_sem=recv,
            device_id={"seq": where},
            device_id_type=MESH,
        )

    def flow_a(h, p):
        return remote(own.at[h, p], buf1.at[h, p], send_a, recv_1.at[h, p], pair)

    def flow_b(h, p):
        return remote(own.at[h, p], buf2.at[h, p], send_b, recv_2.at[h, p], s + 2)

    def flow_c(h, p):
        return remote(buf2.at[h, p], buf1.at[h, p], send_c.at[h, p], recv_1.at[h, p], pair)

    def flow_d(i, p):
        return remote(
            own.at[last - i, p], hop.at[i, p], hop_send.at[i, p], hop_recv.at[i, p], pair
        )

    def flow_e(i, p):
        return remote(
            hop.at[i, p], buf1.at[last - i, p], hop_send.at[i, p], recv_1.at[last - i, p], s + 2
        )

    def ask(i):
        return remote(
            q_own.at[i], q_next.at[i], ask_sem.at[0, i], ask_sem.at[1, i], s - 2
        )

    def answer(i):
        return remote(
            part_out.at[i], part_in.at[i], part_sem.at[0, i], part_sem.at[1, i], s + 2
        )

    def ask_beside():
        return remote(q_own.at[last], q_next.at[0], ask_sem.at[0, 0], ask_sem.at[1, 0], pair)

    def answer_beside():
        return remote(part_out.at[0], part_in.at[0], part_sem.at[0, 0], part_sem.at[1, 0], pair)

    def answer_beside_lse():
        return remote(lse_out.at[0], lse_in.at[0], lse_sem.at[0, 0], lse_sem.at[1, 0], pair)

    def answer_lse(i):
        return remote(lse_out.at[i], lse_in.at[i], lse_sem.at[0, i], lse_sem.at[1, i], s + 2)

    def forwards(h, p):
        return odd & has_prev & (unit(last - h, p) >= skipped)

    def seg_a():
        return remote(seg_ref, seg1, seg_send.at[0], seg_recv.at[0], pair)

    def seg_b():
        return remote(seg_ref, seg2, seg_send.at[1], seg_recv.at[1], s + 2)

    def seg_c():
        return remote(seg2, seg1, seg_send.at[2], seg_recv.at[0], pair)

    def seg_e():
        return remote(seg_ref, seg_beside, seg_send.at[4], seg_recv.at[3], pair)

    def seg_d():
        return remote(seg_ref, seg_next, seg_send.at[3], seg_recv.at[2], s - 2)

    @pl.when(even)
    def _():
        seg_a().start()

    @pl.when(has_next)
    def _():
        seg_b().start()

    @pl.when(asks)
    def _():
        seg_d().start()

        def send_ask(j, carry):
            ask(turn(j, arriving)).start()
            return carry

        lax.fori_loop(0, turns, send_ask, 0)

    @pl.when(ships)
    def _():
        seg_e().start()
        ask_beside().start()

    @pl.when(ships & has_prev)
    def _():
        seg_d().start()
        ask(last).start()

    for i in range(deepest):
        for p in reversed(range(PIECES)):

            @pl.when(unit(i, p) < leaving)
            def _():
                flow_d(i, p).start()

    def send(h, carry):
        for p in range(PIECES):

            @pl.when(has_next & ((odd & ((h < last) | keeps)) | (h < KEPT)))
            def _():
                flow_b(h, p).start()

            @pl.when(even & ((h < last) | keeps))
            def _():
                flow_a(h, p).start()

        return carry

    lax.fori_loop(0, heads, send, 0)

    def arrive(h, pieces):
        for p in pieces:

            @pl.when(s >= 1)
            def _():
                flow_a(h, p).wait_recv()

    def reach(h, p):
        @pl.when(has_prev)
        def _():
            flow_b(h, p).wait_recv()

        @pl.when(forwards(h, p))
        def _():
            flow_c(h, p).start()

    def pass_on(h):
        for p in range(PIECES):
            reach(h, p)

    @pl.when(odd & has_prev)
    def _():
        seg_b().wait_recv()
        seg_c().start()
        pass_on(0)

    @pl.when(s < 1)
    def _():
        buf1[...] = jnp.zeros_like(buf1)
        seg1[...] = jnp.full_like(seg1, -1)

    @pl.when(s < 2)
    def _():
        buf2[...] = jnp.zeros_like(buf2)
        seg2[...] = jnp.full_like(seg2, -1)

    @pl.when(s == 0)
    def _():
        part_in[...] = jnp.zeros_like(part_in)
        lse_in[...] = jnp.full_like(lse_in, NEVER)

    @pl.when(s == 1)
    def _():
        part_in[last] = jnp.zeros((rows, HEAD_DIM), part_in.dtype)
        lse_in[last] = jnp.full((1, rows), NEVER, jnp.float32)

    def column(row):
        return jnp.transpose(jnp.broadcast_to(row, (HEAD_DIM, rows)))

    query_seg = column(seg_ref[...])[:, :1]
    query_pos = lax.broadcasted_iota(jnp.int32, (rows, rows), 0)
    key_pos = lax.broadcasted_iota(jnp.int32, (rows, rows), 1)
    allowed = (query_seg == seg_ref[...]) & (key_pos <= query_pos)
    bias[:, :rows] = jnp.where(allowed, 0.0, -jnp.inf)
    squares[...] = jnp.zeros_like(squares)
    image_ref[...] = column(mod_ref[...])

    def scores_of(query, key):
        return scale * lax.dot_general(
            query, key, (((1,), (1,)), ((), ())), preferred_element_type=jnp.float32
        )

    def relay_head(i):
        for p in reversed(range(PIECES)):

            @pl.when(unit(i, p) < passing)
            def _():
                flow_d(i, p).wait_recv()
                flow_e(i, p).start()

    def attend_for(i, h):
        key = own[h, :half].reshape(rows, HEAD_DIM)
        value = own[h, half:].reshape(rows, HEAD_DIM)
        score = scores_of(q_next[i], key) + bias_next[...]
        top = jnp.max(score, axis=1, keepdims=True)
        weight = jnp.exp(score - top)
        total = jnp.sum(weight, axis=1, keepdims=True)
        acc = jnp.dot(weight.astype(jnp.bfloat16), value, preferred_element_type=jnp.float32)
        part_out[i] = (acc * (1.0 / total)).astype(jnp.bfloat16)
        lse = jnp.broadcast_to(top + jnp.log(total), (rows, HEAD_DIM))
        lse_out[i] = jnp.transpose(lse)[:1]

    def mask_for(ids):
        asker = column(ids[...])[:, :1]
        bias_next[...] = jnp.where(asker == seg_ref[...], 0.0, NEVER)

    def send_answer(i):
        answer_lse(i).start()
        answer(i).start()

    @pl.when(serves)
    def _():
        seg_e().wait_recv()
        mask_for(seg_beside)
        ask_beside().wait_recv()
        attend_for(0, last)

    @pl.when(has_next & (even | ships))
    def _():
        seg_d().wait_recv()
        mask_for(seg_next)

    @pl.when(ships & has_next)
    def _():
        ask(last).wait_recv()
        attend_for(last, last)

    @pl.when(answers)
    def _():
        def attend_next(j, carry):
            h = turn(j, passing)
            ask(h).wait_recv()
            attend_for(h, h)

            @pl.when(j > 0)
            def _():
                send_answer(turn(j - 1, passing))

            @pl.when((lax.rem(j, 2) == 0) & (j // 2 * PIECES < passing))
            def _():
                relay_head(j // 2)

            return carry

        lax.fori_loop(0, turns, attend_next, 0)
        send_answer(turn(turns - 1, passing))

    @pl.when(asks)
    def _():
        seg_b().wait_recv()

    @pl.when(s >= 1)
    def _():
        seg_a().wait_recv()

    bias[:, rows : 2 * rows] = jnp.where(query_seg == seg1[...], 0.0, -jnp.inf)
    bias[:, 2 * rows :] = jnp.where(query_seg == seg2[...], 0.0, -jnp.inf)

    def scores_with(h, block, i):
        key = block[h, :half].reshape(rows, HEAD_DIM)
        return scores_of(q_own[h], key) + bias[:, i * rows : (i + 1) * rows]

    def product(weight, value):
        return jnp.dot(weight.astype(jnp.bfloat16), value, preferred_element_type=jnp.float32)

    def values_of(block, h):
        return block[h, half:].reshape(rows, HEAD_DIM)

    def finish(h, acc, total):
        attended = (acc * (1.0 / total)).astype(jnp.bfloat16)
        att[h] = attended
        wide = attended.astype(jnp.float32)
        return wide * wide

    @pl.when(ships & has_next)
    def _():
        send_answer(last)

    @pl.when(serves)
    def _():
        answer_beside_lse().start()
        answer_beside().start()

    def head(h):
        near = scores_with(h, own, 0)
        far = scores_with(h, buf2, 2)
        arrive(h, range(half))
        middle = scores_with(h, buf1, 1)
        top = jnp.max(jnp.maximum(jnp.maximum(near, middle), far), axis=1, keepdims=True)
        near = jnp.exp(near - top)
        far = jnp.exp(far - top)
        middle = jnp.exp(middle - top)
        total = jnp.sum(near + middle + far, axis=1, keepdims=True)
        acc = product(near, values_of(own, h))

        arrive(h, range(half, PIECES))
        acc = acc + product(far, values_of(buf2, h)) + product(middle, values_of(buf1, h))
        return finish(h, acc, total)

    def joined_last():
        near = scores_with(last, own, 0)
        top = jnp.max(near, axis=1, keepdims=True)
        near = jnp.exp(near - top)
        total = jnp.sum(near, axis=1, keepdims=True)
        acc = product(near, values_of(own, last))

        @pl.when(has_prev)
        def _():
            answer_lse(last).wait_recv()
            answer(last).wait_recv()

        answer_beside_lse().wait_recv()
        answer_beside().wait_recv()
        far_top = column(lse_in[last, :1])[:, :1]
        middle_top = column(lse_in[0, :1])[:, :1]
        most = jnp.maximum(top, jnp.maximum(far_top, middle_top))
        again = jnp.exp(top - most)
        far = jnp.exp(far_top - most)
        middle = jnp.exp(middle_top - most)
        total = again * total + far + middle
        acc = again * acc + far * part_in[last].astype(jnp.float32)
        acc = acc + middle * part_in[0].astype(jnp.float32)
        return finish(last, acc, total)

    def merged(h, apart):
        near = scores_with(h, own, 0)

        @pl.when(asks)
        def _():
            answer_lse(h).wait_recv()
            answer(h).wait_recv()

        lse = column(lse_in[h, :1])[:, :1]
        if not apart:
            arrive(h, range(half))
            middle = scores_with(h, buf1, 1)
            top = jnp.max(jnp.maximum(near, middle), axis=1, keepdims=True)
            top = jnp.maximum(top, lse)
            near = jnp.exp(near - top)
            middle = jnp.exp(middle - top)
            far = jnp.exp(lse - top)
            total = jnp.sum(near + middle, axis=1, keepdims=True) + far
            acc = product(near, values_of(own, h)) + far * part_in[h].astype(jnp.float32)
            arrive(h, range(half, PIECES))
            return finish(h, acc + product(middle, values_of(buf1, h)), total)
        first_top = jnp.maximum(jnp.max(near, axis=1, keepdims=True), lse)
        near = jnp.exp(near - first_top)
        far = jnp.exp(lse - first_top)
        first_total = jnp.sum(near, axis=1, keepdims=True) + far
        acc = product(near, values_of(own, h)) + far * part_in[h].astype(jnp.float32)
        arrive(h, range(half))
        middle = scores_with(h, buf1, 1)
        top = jnp.maximum(jnp.max(middle, axis=1, keepdims=True), first_top)
        middle = jnp.exp(middle - top)
        again = jnp.exp(first_top - top)
        total = jnp.sum(middle, axis=1, keepdims=True) + again * first_total
        acc = acc * again
        arrive(h, range(half, PIECES))
        return finish(h, acc + product(middle, values_of(buf1, h)), total)

    def one(h, carry):
        @pl.when(h + 1 < beside)
        def _():
            pass_on(h + 1)

        @pl.when(h >= beside)
        def _():
            pass_on(h)

        squares[...] += head(h)
        return carry

    def conclude(wide):
        partial = jnp.sum(squares[...] + wide, axis=1, keepdims=True)
        strip = lax.broadcasted_iota(jnp.int32, mine.shape, 1) // (HEAD_DIM // FOLD)
        folded = jnp.broadcast_to(partial[:deep], mine.shape)
        for g in range(1, FOLD):
            folded = jnp.where(strip == g, partial[g * deep : (g + 1) * deep], folded)
        mine[...] = folded

    @pl.when(odd)
    def _():
        lax.fori_loop(0, last, one, 0)

        @pl.when(ships)
        def _():
            conclude(joined_last())

        @pl.when(keeps)
        def _():
            @pl.when(beside < heads)
            def _():
                pass_on(last)

            conclude(head(last))

    def joined(j, carry):
        squares[...] += merged(turn(j, arriving), False)
        return carry

    @pl.when(even)
    def _():
        def kept(h, carry):
            pass_on(h)
            squares[...] += head(h)
            return carry

        lax.fori_loop(0, KEPT, kept, 0)
        lax.fori_loop(0, turns - 1, joined, 0)
        conclude(merged(turn(turns - 1, arriving), True))

    swap = pltpu.make_async_remote_copy(
        src_ref=mine,
        dst_ref=theirs,
        send_sem=sq_sem.at[0],
        recv_sem=sq_sem.at[1],
        device_id={"tp": 1 - t},
        device_id_type=MESH,
    )
    swap.start()

    def sent(ref, send):
        remote(ref, ref, send, recv_1.at[0, 0], pair).wait_send()

    for i in range(deepest):
        for p in range(PIECES):

            @pl.when(unit(i, p) < leaving)
            def _():
                flow_d(i, p).wait_send()

            @pl.when(unit(i, p) < passing)
            def _():
                flow_e(i, p).wait_send()

    @pl.when(asks)
    def _():
        seg_d().wait_send()
        for i in range(KEPT, heads):
            ask(i).wait_send()

    @pl.when(ships)
    def _():
        seg_e().wait_send()
        ask_beside().wait_send()

    @pl.when(ships & has_prev)
    def _():
        seg_d().wait_send()
        ask(last).wait_send()

    @pl.when(ships & has_next)
    def _():
        answer(last).wait_send()
        answer_lse(last).wait_send()

    @pl.when(answers)
    def _():
        for i in range(KEPT, heads):
            answer(i).wait_send()
            answer_lse(i).wait_send()

    @pl.when(even)
    def _():
        seg_a().wait_send()
        sent(own.at[:last], send_a)

    @pl.when(even & keeps)
    def _():
        sent(own.at[last], send_a)

    @pl.when(serves)
    def _():
        answer_beside().wait_send()
        answer_beside_lse().wait_send()

    @pl.when(has_next)
    def _():
        seg_b().wait_send()
        sent(own.at[:KEPT], send_b)

    @pl.when(odd & has_next)
    def _():
        sent(own.at[KEPT:last], send_b)

    @pl.when(odd & has_next & keeps)
    def _():
        sent(own.at[last], send_b)

    @pl.when(odd & has_prev)
    def _():
        seg_c().wait_send()

    for h in range(heads):
        for p in range(PIECES):

            @pl.when(forwards(h, p))
            def _():
                flow_c(h, p).wait_send()

    swap.wait_recv()
    mean_square = (mine[...] + theirs[...]) / (HEADS * HEAD_DIM)
    inverse = lax.rsqrt(mean_square + 1e-05)
    for g in range(FOLD):
        lane = g * (HEAD_DIM // FOLD)
        inverse_ref[g * deep : (g + 1) * deep] = jnp.broadcast_to(
            inverse[:, lane : lane + 1], (deep, HEAD_DIM)
        )
    swap.wait_send()


def blend(heads, att, inverse_ref, image_ref, gain_ref, out_hbm, staged, out_sem):
    inverse = inverse_ref[...]
    image = image_ref[...] == 1
    copies = []
    for h in range(heads):
        columns = slice(h * HEAD_DIM, (h + 1) * HEAD_DIM)
        gain = jnp.where(image, gain_ref[1:2, columns], gain_ref[0:1, columns])
        staged[h] = (att[h].astype(jnp.float32) * inverse * gain).astype(staged.dtype)
        copy = pltpu.make_async_copy(
            staged.at[h], out_hbm.at[:, pl.ds(h * HEAD_DIM, HEAD_DIM)], out_sem.at[h]
        )
        copy.start()
        copies.append(copy)
    for copy in copies:
        copy.wait()


def on_device(n, queries, keys, values, segment_ids, modality, norm_gain):
    rows, width = queries.shape
    heads = width // HEAD_DIM
    vmem = pl.BlockSpec(memory_space=pltpu.VMEM)
    hbm = pl.BlockSpec(memory_space=pltpu.HBM)
    depth = 2 * rows // PIECES
    block = pltpu.VMEM((heads, PIECES, depth, HEAD_DIM), jnp.bfloat16)
    deepest = (max(MOST + LEAST) + PIECES - 1) // PIECES
    asked = pltpu.VMEM((heads, rows, HEAD_DIM), jnp.bfloat16)
    ids = pltpu.VMEM((1, rows), jnp.int32)
    flow = pltpu.SemaphoreType.DMA((heads, PIECES))
    att, inverse, image = pl.pallas_call(
        functools.partial(kernel, n, heads, rows),
        out_shape=(
            pltpu.VMEM((heads, rows, HEAD_DIM), jnp.bfloat16),
            pltpu.VMEM((rows, HEAD_DIM), jnp.float32),
            pltpu.VMEM((rows, HEAD_DIM), jnp.int32),
        ),
        in_specs=[hbm, hbm, hbm, hbm, hbm],
        out_specs=(vmem, vmem, vmem),
        scratch_shapes=[
            pltpu.VMEM((heads, rows, HEAD_DIM), jnp.bfloat16),
            block,
            block,
            block,
            pltpu.VMEM((deepest, PIECES, depth, HEAD_DIM), jnp.bfloat16),
            asked,
            asked,
            pltpu.VMEM((heads, 1, rows), jnp.float32),
            asked,
            pltpu.VMEM((heads, 1, rows), jnp.float32),
            ids,
            ids,
            ids,
            ids,
            ids,
            ids,
            pltpu.VMEM((rows, (REACH + 1) * rows), jnp.float32),
            pltpu.VMEM((rows, rows), jnp.float32),
            pltpu.VMEM((rows, HEAD_DIM), jnp.float32),
            pltpu.VMEM((rows // FOLD, HEAD_DIM), jnp.float32),
            pltpu.VMEM((rows // FOLD, HEAD_DIM), jnp.float32),
            pltpu.SemaphoreType.DMA,
            pltpu.SemaphoreType.DMA,
            pltpu.SemaphoreType.DMA,
            pltpu.SemaphoreType.DMA,
            flow,
            flow,
            flow,
            pltpu.SemaphoreType.DMA((deepest, PIECES)),
            pltpu.SemaphoreType.DMA((deepest, PIECES)),
            pltpu.SemaphoreType.DMA((2, heads)),
            pltpu.SemaphoreType.DMA((2, heads)),
            pltpu.SemaphoreType.DMA((2, heads)),
            pltpu.SemaphoreType.DMA((2,)),
            pltpu.SemaphoreType.DMA((5,)),
            pltpu.SemaphoreType.DMA((4,)),
            pltpu.SemaphoreType.DMA((2,)),
        ],
        compiler_params=pltpu.CompilerParams(
            collective_id=0, has_side_effects=True
        ),
    )(queries, keys, values, segment_ids.reshape(1, rows), modality.reshape(1, rows))
    return pl.pallas_call(
        functools.partial(blend, heads),
        out_shape=jax.ShapeDtypeStruct((rows, width), jnp.bfloat16),
        in_specs=[vmem, vmem, vmem, vmem],
        out_specs=hbm,
        scratch_shapes=[
            pltpu.VMEM((heads, rows, HEAD_DIM), jnp.bfloat16),
            pltpu.SemaphoreType.DMA((heads,)),
        ],
        compiler_params=pltpu.CompilerParams(vmem_limit_bytes=8 * 2**20),
    )(att, inverse, image, norm_gain)


def solution(mesh):
    return jax.shard_map(
        functools.partial(on_device, mesh.shape["seq"]),
        mesh=mesh,
        in_specs=(
            P(("grp", "seq"), "tp"),
            P(("grp", "seq"), "tp"),
            P(("grp", "seq"), "tp"),
            P(("grp", "seq")),
            P(("grp", "seq")),
            P(None, "tp"),
        ),
        out_specs=P(("grp", "seq"), "tp"),
        check_vma=False,
    )
```
